32 devices in a mesh: pp: 4 (over z), dp: 8 (over y, x, core).
Axes of the slice: x: 2, y: 2, z: 4, core: 2. Of those that a mesh axis runs over, the one named last changes fastest.
Arguments:
- tok_ids: int32 [4, 256], P(None, 'dp')
- d_out: bfloat16 [4, 256, 512], P('pp', 'dp')
- stored_x: bfloat16 [4, 4, 256, 512], P('pp', None, 'dp')
- w_in: bfloat16 [12, 512, 2048], P('pp')
- w_out: bfloat16 [12, 2048, 512], P('pp')
- acc_in: float32 [12, 8, 512, 2048], P('pp', 'dp')
- acc_out: float32 [12, 8, 2048, 512], P('pp', 'dp')
- acc_emb: float32 [8, 30522, 512], P('dp')
Outputs:
- output 1: float32 [12, 512, 2048], P('pp', 'dp')
- output 2: float32 [12, 2048, 512], P('pp', 'dp')
- output 3: float32 [30522, 512], P(None, 'dp')
All inputs are finite; a program needn't handle non-finite values.
Results may differ from the reference program's by a relative error of at most 0.01615.
Values are sent between devices in bfloat16 or wider.
A program may use at most 1 GiB of HBM per device.

```python
import jax
import jax.numpy as jnp
from jax import lax

STAGES = 4
REPLICAS = 8
LAYERS = 3
HID = 512
FF = 2048
VOCAB = 30522
TOKENS_DEV = 32

ROWS_ALL = TOKENS_DEV * REPLICAS


def setup_inputs(seed: int = 0) -> dict:
    key_list = jax.random.split(jax.random.key(seed), 8)
    tok_ids = jax.random.randint(key_list[0], (STAGES, ROWS_ALL), 0, VOCAB, dtype=jnp.int32)
    d_out = jax.random.normal(key_list[1], (STAGES, ROWS_ALL, HID), jnp.float32).astype(jnp.bfloat16)
    stored_x = jax.random.normal(key_list[2], (STAGES, STAGES, ROWS_ALL, HID), jnp.float32).astype(jnp.bfloat16)
    w_in = (jax.random.normal(key_list[3], (STAGES * LAYERS, HID, FF), jnp.float32) * HID ** -0.5).astype(jnp.bfloat16)
    w_out = (jax.random.normal(key_list[4], (STAGES * LAYERS, FF, HID), jnp.float32) * (FF * STAGES * LAYERS) ** -0.5).astype(jnp.bfloat16)
    in_scale = 0.2 * (TOKENS_DEV / LAYERS) ** 0.5
    out_scale = 0.4 * (TOKENS_DEV * STAGES) ** 0.5
    acc_in = jax.random.normal(key_list[5], (STAGES * LAYERS, REPLICAS, HID, FF), jnp.float32) * in_scale
    acc_out = jax.random.normal(key_list[6], (STAGES * LAYERS, REPLICAS, FF, HID), jnp.float32) * out_scale
    acc_emb = jax.random.normal(key_list[7], (REPLICAS, VOCAB, HID), jnp.float32) * 0.5
    return {'tok_ids': tok_ids, 'd_out': d_out, 'stored_x': stored_x, 'w_in': w_in, 'w_out': w_out, 'acc_in': acc_in, 'acc_out': acc_out, 'acc_emb': acc_emb}


def layer_forward(x_cur, w_in_l, w_out_l):
    pre_act = jnp.dot(x_cur, w_in_l, preferred_element_type=jnp.float32).astype(jnp.bfloat16)
    hidden = jax.nn.gelu(pre_act.astype(jnp.float32)).astype(jnp.bfloat16)
    out_x = (x_cur.astype(jnp.float32) + jnp.dot(hidden, w_out_l, preferred_element_type=jnp.float32)).astype(jnp.bfloat16)
    return out_x, pre_act, hidden


def per_replica(left_rows, right_rows):
    left_r = left_rows.reshape(REPLICAS, TOKENS_DEV, left_rows.shape[-1]).astype(jnp.float32)
    right_r = right_rows.reshape(REPLICAS, TOKENS_DEV, right_rows.shape[-1]).astype(jnp.float32)
    return jnp.einsum('rti,rtf->rif', left_r, right_r)


def stage_backward(w_in_s, w_out_s, acc_in_s, acc_out_s, x_stage, cot_stage):
    def one_micro(carry, item):
        sum_in, sum_out = carry
        x_first, cot_first = item

        def fwd_step(x_cur, weights):
            out_x, pre_act, hidden = layer_forward(x_cur, weights[0], weights[1])
            return out_x, (x_cur, pre_act, hidden)

        _, saved_acts = lax.scan(fwd_step, x_first, (w_in_s, w_out_s))

        def bwd_step(cot_cur, layer_item):
            w_in_l, w_out_l, x_cur, pre_act, hidden = layer_item
            g_out = per_replica(hidden, cot_cur)
            d_hidden = jnp.dot(cot_cur, w_out_l.T, preferred_element_type=jnp.float32).astype(jnp.bfloat16)
            pre_f = pre_act.astype(jnp.float32)
            gelu_slope = jax.jvp(jax.nn.gelu, (pre_f,), (jnp.ones_like(pre_f),))[1]
            d_pre = (d_hidden.astype(jnp.float32) * gelu_slope).astype(jnp.bfloat16)
            g_in = per_replica(x_cur, d_pre)
            d_x = (cot_cur.astype(jnp.float32) + jnp.dot(d_pre, w_in_l.T, preferred_element_type=jnp.float32)).astype(jnp.bfloat16)
            return d_x, (g_in, g_out)

        d_first, grads = lax.scan(bwd_step, cot_first, (w_in_s, w_out_s) + saved_acts, reverse=True)
        return (sum_in + grads[0], sum_out + grads[1]), d_first

    sums, d_cots = lax.scan(one_micro, (acc_in_s, acc_out_s), (x_stage, cot_stage))
    return sums[0], sums[1], d_cots


def replica_mean(total, axis_pos):
    return jnp.sum(total.astype(jnp.bfloat16).astype(jnp.float32), axis=axis_pos) / REPLICAS


def reference(tok_ids, d_out, stored_x, w_in, w_out, acc_in, acc_out, acc_emb):
    grads_in = []
    grads_out = []
    cot_rows = d_out[:0]
    for stage_id in range(STAGES - 1, -1, -1):
        pending = STAGES - stage_id
        first_row = stage_id * LAYERS
        last_row = first_row + LAYERS
        cot_rows = jnp.concatenate([cot_rows, d_out[stage_id:stage_id + 1]], axis=0)
        sum_in, sum_out, cot_rows = stage_backward(w_in[first_row:last_row], w_out[first_row:last_row], acc_in[first_row:last_row], acc_out[first_row:last_row], stored_x[stage_id, :pending], cot_rows)
        grads_in = [replica_mean(sum_in, 1)] + grads_in
        grads_out = [replica_mean(sum_out, 1)] + grads_out
    row_replica = jnp.arange(ROWS_ALL, dtype=jnp.int32) // TOKENS_DEV
    segment_ids = (tok_ids + row_replica[None, :] * VOCAB).reshape(-1)
    emb_new = jax.ops.segment_sum(cot_rows.reshape(-1, HID).astype(jnp.float32), segment_ids, num_segments=REPLICAS * VOCAB)
    grad_emb = replica_mean(acc_emb + emb_new.reshape(REPLICAS, VOCAB, HID), 0)
    return (jnp.concatenate(grads_in, axis=0), jnp.concatenate(grads_out, axis=0), grad_emb)
```

```python
import functools

import jax
import jax.numpy as jnp
from jax import lax
from jax.experimental import pallas as pl
from jax.experimental.pallas import tpu as pltpu
from jax.sharding import PartitionSpec as P

MESH_ID = pl.DeviceIdType.MESH
BF = jnp.bfloat16
F32 = jnp.float32

VOCAB_CHUNK = 768
CHUNKS = 5
HALF_VOCAB = VOCAB_CHUNK * CHUNKS
WEIGHT_UNITS = 6
UNIT_ORDER = (('w', 0), ('e', 0), ('e', 1), ('e', 2), ('e', 3), ('e', 4), ('w', 1), ('w', 2), ('w', 3), ('w', 4), ('w', 5))
LAG_ADD, LAG_SECOND, LAG_LAST = 1, 3, 5


def layer_forward(x_cur, w_in_l, w_out_l):
    pre_act = jnp.dot(x_cur, w_in_l, preferred_element_type=F32).astype(BF)
    hidden = jax.nn.gelu(pre_act.astype(F32)).astype(BF)
    out_x = (x_cur.astype(F32) + jnp.dot(hidden, w_out_l, preferred_element_type=F32)).astype(BF)
    return out_x, pre_act, hidden


def chain_xla(d_out, stored_x, w_in, w_out, stages):
    stage_id = lax.axis_index('pp')
    layers = w_in.shape[0]
    rows = d_out.shape[1]
    x_steps = []
    for step_id in range(stages):
        micro_id = jnp.maximum(stages - 1 - stage_id - step_id, 0)
        x_steps.append(lax.dynamic_index_in_dim(stored_x[0], micro_id, axis=0, keepdims=False))
    x_cur = jnp.concatenate(x_steps, axis=0)
    saved = []
    for layer_id in range(layers):
        out_x, pre_act, hidden = layer_forward(x_cur, w_in[layer_id], w_out[layer_id])
        slope = jax.jvp(jax.nn.gelu, (pre_act.astype(F32),), (jnp.ones(pre_act.shape, F32),))[1]
        saved.append((x_cur, hidden, slope))
        x_cur = out_x
    g_all = [[None] * stages for _ in range(layers)]
    dh_all = [[None] * stages for _ in range(layers)]
    dx_all = []
    cot = d_out[0]
    for step_id in range(stages):
        sl = slice(step_id * rows, (step_id + 1) * rows)
        for layer_id in range(layers - 1, -1, -1):
            g_all[layer_id][step_id] = cot
            d_hidden = lax.dot_general(cot, w_out[layer_id], (((1,), (1,)), ((), ())), preferred_element_type=F32).astype(BF)
            d_pre = (d_hidden.astype(F32) * saved[layer_id][2][sl]).astype(BF)
            dh_all[layer_id][step_id] = d_pre
            back = lax.dot_general(d_pre, w_in[layer_id], (((1,), (1,)), ((), ())), preferred_element_type=F32)
            cot = (cot.astype(F32) + back).astype(BF)
        dx_all.append(cot)
        if step_id < stages - 1:
            cot = lax.ppermute(cot, 'pp', [(sender, sender - 1) for sender in range(1, stages)])
    xs = jnp.stack([s[0] for s in saved])
    hs = jnp.stack([s[1] for s in saved])
    gs = jnp.stack([jnp.concatenate(r, axis=0) for r in g_all])
    dhs = jnp.stack([jnp.concatenate(r, axis=0) for r in dh_all])
    return xs, hs, gs, dhs, jnp.concatenate(dx_all, axis=0)


def ag_events():
    events = [(k, hop) for k in range(CHUNKS) for hop in (1, 2, 3)]
    return sorted(events, key=lambda e: (e[0] + e[1], e[1]))


def comm_kernel(stages, vocab, ids_ref, dx_ref, x_ref, h_ref, g_ref, dh_ref, acc_in, acc_out, acc_emb,
                gin_ref, gout_ref, emb_ref,
                u_in, r0_in, r1_in, r2_in, u_out, r0_out, r1_out, r2_out, u_e, r0_e, r1_e, r2_e,
                ag, dxb, st_in, st_out, st_e, st_t,
                sem_st_in, sem_st_out, sem_st_e, sem_t, s0s, s0r, s1s, s1r, s2s, s2r,
                dxs, dxr, up_s, dn_s, pt_s, col_r, pt_r):
    s = lax.axis_index('pp')
    d = lax.axis_index('dp')
    c = lax.rem(d, 2)
    x = lax.rem(d // 2, 2)
    y = d // 4
    core_peer = d + 1 - 2 * c
    x_peer = d + 2 - 4 * x
    y_peer = d + 4 - 8 * y
    last = stages - 1

    def send(src, dst, ss, rs, target):
        return pltpu.make_async_remote_copy(src_ref=src, dst_ref=dst, send_sem=ss, recv_sem=rs, device_id=target, device_id_type=MESH_ID)

    barrier = pltpu.get_barrier_semaphore()
    for peer in (core_peer, x_peer, y_peer):
        pl.semaphore_signal(barrier, inc=1, device_id=(s, peer), device_id_type=MESH_ID)
    for off in range(1, stages):
        pl.semaphore_signal(barrier, inc=1, device_id=(lax.rem(s + off, stages), d), device_id_type=MESH_ID)

    def in_copy(n):
        unit, yx = n // 4, lax.rem(n, 4)
        slot = lax.rem(n, 2)
        return pltpu.make_async_copy(acc_in.at[unit, pl.ds(yx * 128, 128), :], st_in.at[slot], sem_st_in.at[slot])

    def out_copy(n):
        unit, yx = n // 4, lax.rem(n, 4)
        slot = lax.rem(n, 2)
        return pltpu.make_async_copy(acc_out.at[unit, pl.ds(yx * 512, 512), :], st_out.at[slot], sem_st_out.at[slot])

    part_rows = HALF_VOCAB * 4
    chunk_rows = VOCAB_CHUNK * 4
    tail_rows = vocab * 4 - (part_rows * 2 * stages - chunk_rows)

    def emb_copy(n, act):
        k, half = n // 2, n % 2
        slot = n % 2
        start = pl.multiple_of(s * (2 * part_rows) + half * part_rows + k * chunk_rows, 8)

        def full():
            act(pltpu.make_async_copy(acc_emb.at[pl.ds(start, chunk_rows), :], st_e.at[slot], sem_st_e.at[slot]))

        if k == CHUNKS - 1 and half == 1:
            @pl.when(s == last)
            def _():
                act(pltpu.make_async_copy(acc_emb.at[pl.ds(vocab * 4 - tail_rows, tail_rows), :],
                                          st_e.at[slot, pl.ds(0, tail_rows), :], sem_st_e.at[slot]))

            @pl.when(s != last)
            def _():
                full()
        else:
            full()

    for n in range(2):
        in_copy(jnp.int32(n)).start()
        out_copy(jnp.int32(n)).start()
        emb_copy(n, lambda cp: cp.start())

    pl.semaphore_wait(barrier, 3 + stages - 1)

    @pl.when(s == 0)
    def _():
        for z in range(1, stages):
            send(dx_ref, dxb, dxs.at[z], dxr, (z, d)).start()
        for q in range(4):
            dxb[q] = dx_ref[q]

    def weight_produce(unit):
        layer = unit // 2
        if unit % 2 == 0:
            def body(yx, carry):
                n = 4 * layer + yx
                slot = lax.rem(n, 2)
                in_copy(n).wait()
                lhs = x_ref[layer, :, pl.ds(pl.multiple_of(yx * 128, 128), 128)]
                for col in range(4):
                    cs = slice(col * 512, (col + 1) * 512)
                    new = lax.dot_general(lhs, dh_ref[layer, :, cs], (((0,), (0,)), ((), ())), preferred_element_type=F32)
                    tot = (st_in[slot, :, cs] + new).astype(BF)
                    u_in[layer, yx, 0, :, cs] = tot[:64]
                    u_in[layer, yx, 1, :, cs] = tot[64:]

                @pl.when(n + 2 < 12)
                def _():
                    in_copy(n + 2).start()
                return carry
        else:
            def body(yx, carry):
                n = 4 * layer + yx
                slot = lax.rem(n, 2)
                out_copy(n).wait()
                for part in range(4):
                    rows = pl.ds(part * 128, 128)
                    lhs = h_ref[layer, :, pl.ds(pl.multiple_of(yx * 512 + part * 128, 128), 128)]
                    new = lax.dot_general(lhs, g_ref[layer], (((0,), (0,)), ((), ())), preferred_element_type=F32)
                    tot = (st_out[slot, rows, :] + new).astype(BF)
                    u_out[layer, yx, part // 2, pl.ds((part % 2) * 128, 128), :] = tot

                @pl.when(n + 2 < 12)
                def _():
                    out_copy(n + 2).start()
                return carry
        lax.fori_loop(0, 4, body, 0)

    def emb_produce(k):
        if k == 0:
            @pl.when(s > 0)
            def _():
                send(dx_ref, dxb, dxs.at[0], dxr, (0, d)).wait_recv()
        for half in range(2):
            n = 2 * k + half
            emb_copy(n, lambda cp: cp.wait())
            base = s * (2 * HALF_VOCAB) + half * HALF_VOCAB + k * VOCAB_CHUNK
            hot = (lax.broadcasted_iota(jnp.int32, (VOCAB_CHUNK, 128), 0) + base == ids_ref[...]).astype(F32).astype(BF)

            def body(q, carry):
                new = jnp.dot(hot, dxb[q], preferred_element_type=F32)
                old = st_e[n % 2, pl.ds(q, VOCAB_CHUNK, stride=4), :]
                u_e[k, q, half] = (old + new).astype(BF)
                return carry
            lax.fori_loop(0, 4, body, 0)
            if n + 2 < 2 * CHUNKS:
                emb_copy(n + 2, lambda cp: cp.start())

    def unit_bufs(kind, i):
        if kind == 'e':
            return u_e.at[i], r0_e.at[i], r1_e.at[i], r2_e.at[i], VOCAB_CHUNK
        if i % 2 == 0:
            return u_in.at[i // 2], r0_in.at[i // 2], r1_in.at[i // 2], r2_in.at[i // 2], 64
        return u_out.at[i // 2], r0_out.at[i // 2], r1_out.at[i // 2], r2_out.at[i // 2], 256

    def add_into(u, idx, r, ridx):
        u[idx] = u[idx] + r[ridx]

    def core_send(pos):
        u, r0, r1, r2, rows = unit_bufs(*UNIT_ORDER[pos])
        return send(u.at[:, 1 - c], r0, s0s.at[pos], s0r.at[pos], (s, core_peer))

    def first_send(pos):
        u, r0, r1, r2, rows = unit_bufs(*UNIT_ORDER[pos])
        if pos % 2 == 0:
            return [send(u.at[2 * j + 1 - x, c], r1.at[j], s1s.at[pos, j], s1r.at[pos, j], (s, x_peer)) for j in range(2)]
        return [send(u.at[2 * (1 - y) + j, c], r1.at[j], s1s.at[pos, j], s1r.at[pos, j], (s, y_peer)) for j in range(2)]

    def second_send(pos):
        u, r0, r1, r2, rows = unit_bufs(*UNIT_ORDER[pos])
        if pos % 2 == 0:
            return send(u.at[2 * (1 - y) + x, c], r2, s2s.at[pos], s2r.at[pos], (s, y_peer))
        return send(u.at[2 * y + 1 - x, c], r2, s2s.at[pos], s2r.at[pos], (s, x_peer))

    def stage_produce(pos):
        kind, i = UNIT_ORDER[pos]
        if kind == 'w':
            weight_produce(i)
        else:
            emb_produce(i)
        core_send(pos).start()

    def stage_add(pos):
        u, r0, r1, r2, rows = unit_bufs(*UNIT_ORDER[pos])
        core_send(pos).wait_recv()
        sends = first_send(pos)
        order = ([2 * j + 1 - x for j in range(2)] + [2 * j + x for j in range(2)]) if pos % 2 == 0 else \
                ([2 * (1 - y) + j for j in range(2)] + [2 * y + j for j in range(2)])
        for j, blk in enumerate(order):
            u[blk, c] = u[blk, c] + r0[blk]
            if j < 2:
                sends[j].start()

    def stage_second(pos):
        u, r0, r1, r2, rows = unit_bufs(*UNIT_ORDER[pos])
        for cp in first_send(pos):
            cp.wait_recv()
        if pos % 2 == 0:
            far, near = (2 * (1 - y) + x, 1 - y), (2 * y + x, y)
        else:
            far, near = (2 * y + 1 - x, 1 - x), (2 * y + x, x)
        u[far[0], c] = u[far[0], c] + r1[far[1]]
        second_send(pos).start()
        u[near[0], c] = u[near[0], c] + r1[near[1]]

    def col_send(z, k, sem, target_s):
        piece = ag.at[2 * z + c, k]
        return send(piece, piece, sem.at[z, k], col_r.at[z, k], (target_s, d))

    def part_send(z, k):
        piece = ag.at[2 * z + c, k]
        return send(piece, piece, pt_s.at[z, k], pt_r.at[z, k], (s, core_peer))

    counter = [0]
    sel = (lax.broadcasted_iota(jnp.int32, (64, 128), 1) == lax.broadcasted_iota(jnp.int32, (64, 128), 0) + 64 * c).astype(F32).astype(BF)

    def out_copy_t(slot, p, k):
        start = pl.multiple_of(p * HALF_VOCAB + k * VOCAB_CHUNK, 128)
        return pltpu.make_async_copy(st_t.at[slot], emb_ref.at[:, pl.ds(start, VOCAB_CHUNK)], sem_t.at[slot])

    def emit(p, k):
        st_t[k, p] = lax.dot_general(sel, ag[p, k], (((1,), (1,)), ((), ())), preferred_element_type=F32).astype(BF)
        pltpu.make_async_copy(st_t.at[k, p], emb_ref.at[:, pl.ds(pl.multiple_of(p * HALF_VOCAB + k * VOCAB_CHUNK, 128), VOCAB_CHUNK)],
                              sem_t.at[k, p]).start()

    def have_piece(z, k, go_up, go_down):
        if go_up:
            @pl.when(s < last)
            def _():
                col_send(z, k, up_s, s + 1).start()
        if go_down:
            @pl.when(s > 0)
            def _():
                col_send(z, k, dn_s, s - 1).start()
        part_send(z, k).start()
        emit(2 * z + c, k)

    def stage_last(pos):
        kind, i = UNIT_ORDER[pos]
        u, r0, r1, r2, rows = unit_bufs(kind, i)
        second_send(pos).wait_recv()
        mine = 2 * y + x
        if kind == 'e':
            ag[2 * s + c, i] = u[mine, c] + r2[...]
            have_piece(s, i, True, True)
        else:
            tot = (u[mine, c].astype(F32) + r2[...].astype(F32))
            if i % 2 == 0:
                gin_ref[i // 2] = tot
            else:
                gout_ref[i // 2] = tot

    def part_event(z, k):
        part_send(z, k).wait_recv()
        emit(2 * z + 1 - c, k)

    def hop_event(k, hop):
        @pl.when(s - hop >= 0)
        def _():
            z = jnp.maximum(s - hop, 0)
            col_send(z, k, up_s, s).wait_recv()
            have_piece(z, k, True, False)

        @pl.when(s + hop <= last)
        def _():
            z = jnp.minimum(s + hop, last)
            col_send(z, k, dn_s, s).wait_recv()
            have_piece(z, k, False, True)

    events = ag_events()
    total = len(UNIT_ORDER)
    for tick in range(total + LAG_LAST):
        if tick < total:
            stage_produce(tick)
        if 0 <= tick - LAG_ADD < total:
            stage_add(tick - LAG_ADD)
        if 0 <= tick - LAG_SECOND < total:
            stage_second(tick - LAG_SECOND)
        if 0 <= tick - LAG_LAST < total:
            stage_last(tick - LAG_LAST)
        if tick >= 8:
            for _ in range(2):
                if events and events[0][0] <= tick - LAG_LAST - 1:
                    hop_event(*events.pop(0))
    while events:
        hop_event(*events.pop(0))

    def drain_part(i, carry):
        part_event(i // CHUNKS, lax.rem(i, CHUNKS))
        return carry
    lax.fori_loop(0, stages * CHUNKS, drain_part, 0)

    for pos in range(total):
        core_send(pos).wait_send()
        for cp in first_send(pos):
            cp.wait_send()
        second_send(pos).wait_send()

    @pl.when(s == 0)
    def _():
        for z in range(1, stages):
            send(dx_ref, dxb, dxs.at[z], dxr, (z, d)).wait_send()

    def drain(i, carry):
        z, k = i // CHUNKS, lax.rem(i, CHUNKS)
        part_send(z, k).wait_send()

        @pl.when((z <= s) & (s < last))
        def _():
            col_send(z, k, up_s, jnp.minimum(s + 1, last)).wait_send()

        @pl.when((z >= s) & (s > 0))
        def _():
            col_send(z, k, dn_s, jnp.maximum(s - 1, 0)).wait_send()
        for core in range(2):
            pltpu.make_async_copy(st_t.at[k, 2 * z + core], emb_ref.at[:, pl.ds(0, VOCAB_CHUNK)], sem_t.at[k, 2 * z + core]).wait()
        return carry
    lax.fori_loop(0, stages * CHUNKS, drain, 0)


def solution(mesh):
    stages = mesh.shape['pp']
    replicas = mesh.shape['dp']

    def device_body(tok_ids, d_out, stored_x, w_in, w_out, acc_in, acc_out, acc_emb):
        layers, hid, ff = w_in.shape
        vocab = acc_emb.shape[1]
        xs, hs, gs, dhs, dx = chain_xla(d_out, stored_x, w_in, w_out, stages)
        rows = dx.shape[0]
        ids = tok_ids[::-1].reshape(1, rows)
        dx_q = dx.reshape(rows, 4, 128).transpose(1, 0, 2)
        v = pltpu.VMEM
        dma = pltpu.SemaphoreType.DMA
        units = len(UNIT_ORDER)
        vm = pl.BlockSpec(memory_space=pltpu.VMEM)
        hbm = pl.BlockSpec(memory_space=pltpu.HBM)
        gin, gout, emb = pl.pallas_call(
            functools.partial(comm_kernel, stages, vocab),
            out_shape=(jax.ShapeDtypeStruct((layers, hid // 8, ff), F32), jax.ShapeDtypeStruct((layers, ff // 8, hid), F32),
                       jax.ShapeDtypeStruct((64, HALF_VOCAB * 2 * stages), BF)),
            in_specs=[vm] * 6 + [hbm] * 3,
            out_specs=(vm, vm, hbm),
            scratch_shapes=[
                v((layers, 4, 2, 64, ff), BF), v((layers, 4, 64, ff), BF), v((layers, 2, 64, ff), BF), v((layers, 64, ff), BF),
                v((layers, 4, 2, 256, hid), BF), v((layers, 4, 256, hid), BF), v((layers, 2, 256, hid), BF), v((layers, 256, hid), BF),
                v((CHUNKS, 4, 2, VOCAB_CHUNK, 128), BF), v((CHUNKS, 4, VOCAB_CHUNK, 128), BF), v((CHUNKS, 2, VOCAB_CHUNK, 128), BF), v((CHUNKS, VOCAB_CHUNK, 128), BF),
                v((2 * stages, CHUNKS, VOCAB_CHUNK, 128), BF), v((4, rows, 128), BF),
                v((2, 128, ff), F32), v((2, 512, hid), F32), v((2, VOCAB_CHUNK * 4, 128), F32), v((CHUNKS, 2 * stages, 64, VOCAB_CHUNK), BF),
                dma((2,)), dma((2,)), dma((2,)), dma((CHUNKS, 2 * stages)),
                dma((units,)), dma((units,)), dma((units, 2)), dma((units, 2)), dma((units,)), dma((units,)),
                dma((stages,)), dma, dma((stages, CHUNKS)), dma((stages, CHUNKS)), dma((stages, CHUNKS)), dma((stages, CHUNKS)), dma((stages, CHUNKS)),
            ],
            compiler_params=pltpu.CompilerParams(collective_id=0, has_side_effects=True, vmem_limit_bytes=67043328),
            name='reduce_exchange',
        )(ids, dx_q, xs, hs, gs, dhs, acc_in.reshape(layers, hid, ff), acc_out.reshape(layers, ff, hid), acc_emb.reshape(vocab * 4, 128))
        scale = 1.0 / replicas
        grad_emb = (emb[:, :vocab].astype(F32) * scale).T
        return gin * scale, gout * scale, grad_emb

    return jax.shard_map(device_body, mesh=mesh, in_specs=(P(None, 'dp'), P('pp', 'dp', None), P('pp', None, 'dp', None), P('pp', None, None), P('pp', None, None), P('pp', 'dp', None, None), P('pp', 'dp', None, None), P('dp', None, None)), out_specs=(P('pp', 'dp', None), P('pp', 'dp', None), P(None, 'dp')), check_vma=False)
```

```python
import functools

import jax
import jax.numpy as jnp
from jax import lax
from jax.experimental import pallas as pl
from jax.experimental.pallas import tpu as pltpu
from jax.sharding import PartitionSpec as P

MESH_ID = pl.DeviceIdType.MESH
BF = jnp.bfloat16
F32 = jnp.float32

VOCAB_CHUNK = 768
CHUNKS = 5
HALF_VOCAB = VOCAB_CHUNK * CHUNKS
WEIGHT_UNITS = 6
FINISH_BLOCK = 6144
UNIT_ORDER = tuple(('e', i) for i in range(CHUNKS)) + (('w', 5), ('w', 4), ('t', 0), ('w', 3), ('w', 2), ('w', 1), ('w', 0))
GROUPS = ((0, 1), (1, 1), (2, 1), (3, 1), (4, 1))
TOUCH_GROUP = len(GROUPS)
CHAIN_SLOTS = ('p0', 'p1', 'a0 p2', 'a1 p3', 'a2 p4', 'a3', '', '', '', 's0 a4 s1', '', '', 's2 s3', '', 'l0', 's4 l2', 'l1 p5 l4 p6 l3', 'a5', 'a6 h p7 p8 a7')
TAIL_SLOTS = ('h p9 p10 h h a8 p11 a9 s5 s7 h h s6', 'a11 a10 h h s9 s8 h', 'l6 l5 l7 h', 's11 s10 h h h', 'l8 l9 h', 'l10 h', 'l11')


def gelu_and_slope(pre):
    return jax.jvp(jax.nn.gelu, (pre,), (jnp.ones_like(pre),))


def comm_kernel(stages, layers, vocab, ids_ref, slot_ref, touched_ref, cot_ref, stored_ref, w_in, w_out, acc_in, acc_out, acc_emb,
                gin_ref, gout_ref, emb_ref, patch_ref, x_ref, h_ref, g_ref, dh_ref, slope, cot_buf, cot_rcv,
                sem_w, sem_cs, sem_cr,
                u_in, r0_in, r1_in, r2_in, u_out, r0_out, r1_out, r2_out, u_e, r0_e, r1_e, r2_e, u_t, r0_t, r1_t, r2_t,
                ag, agt, dxb, st_in, st_out, st_e,
                sem_st_in, sem_st_out, sem_st_e, sem_t, s0s, s0r, s1s, s1r, s2s, s2r,
                dxs, dxr, own_s, fwd_s, pt_s, col_r, pt_r):
    s = lax.axis_index('pp')
    d = lax.axis_index('dp')
    c = lax.rem(d, 2)
    x = lax.rem(d // 2, 2)
    y = d // 4
    core_peer = d + 1 - 2 * c
    x_peer = d + 2 - 4 * x
    y_peer = d + 4 - 8 * y
    last = stages - 1

    def send(src, dst, ss, rs, target):
        return pltpu.make_async_remote_copy(src_ref=src, dst_ref=dst, send_sem=ss, recv_sem=rs, device_id=target, device_id_type=MESH_ID)

    barrier = pltpu.get_barrier_semaphore()
    for peer in (core_peer, x_peer, y_peer):
        pl.semaphore_signal(barrier, inc=1, device_id=(s, peer), device_id_type=MESH_ID)
    for off in range(1, stages):
        pl.semaphore_signal(barrier, inc=1, device_id=(lax.rem(s + off, stages), d), device_id_type=MESH_ID)

    def in_copy(n):
        unit, yx = n // 4, lax.rem(n, 4)
        slot = lax.rem(n, 2)
        return pltpu.make_async_copy(acc_in.at[layers - 1 - unit, pl.ds(yx * 128, 128), :], st_in.at[slot], sem_st_in.at[slot])

    def out_copy(n):
        unit, yx = n // 4, lax.rem(n, 4)
        slot = lax.rem(n, 2)
        return pltpu.make_async_copy(acc_out.at[layers - 1 - unit, pl.ds(yx * 512, 512), :], st_out.at[slot], sem_st_out.at[slot])

    part_rows = HALF_VOCAB * 4
    chunk_rows = VOCAB_CHUNK * 4
    tail_rows = vocab * 4 - (part_rows * 2 * stages - chunk_rows)

    def emb_copy(n, act):
        k, half = n // 2, n % 2
        slot = n % 2
        start = pl.multiple_of(s * (2 * part_rows) + half * part_rows + k * chunk_rows, 8)

        def full():
            act(pltpu.make_async_copy(acc_emb.at[pl.ds(start, chunk_rows), :], st_e.at[slot], sem_st_e.at[slot]))

        if k == CHUNKS - 1 and half == 1:
            @pl.when(s == last)
            def _():
                act(pltpu.make_async_copy(acc_emb.at[pl.ds(vocab * 4 - tail_rows, tail_rows), :],
                                          st_e.at[slot, pl.ds(0, tail_rows), :], sem_st_e.at[slot]))

            @pl.when(s != last)
            def _():
                full()
        else:
            full()

    w_copies = []
    for layer in range(layers):
        for j, (w, u) in enumerate(((w_in, u_in), (w_out, u_out))):
            w_copies.append(pltpu.make_async_copy(w.at[layer], u.at[layer], sem_w.at[2 * layer + j]))
            w_copies[-1].start()
    for n in range(2):
        in_copy(jnp.int32(n)).start()
        out_copy(jnp.int32(n)).start()
        emb_copy(n, lambda cp: cp.start())

    rows = cot_ref.shape[0]

    def dx_send(k, z):
        return send(dxb.at[k], dxb.at[k], dxs.at[k, z], dxr.at[k], (z, d))

    def cot_send(k, target):
        return send(cot_buf.at[k], cot_rcv.at[k], sem_cs.at[k], sem_cr.at[k], (target, d))

    def weight_produce(unit):
        layer = unit // 2
        if unit % 2 == 0:
            def body(yx, carry):
                n = 4 * (layers - 1 - layer) + yx
                slot = lax.rem(n, 2)
                in_copy(n).wait()
                lhs = x_ref[layer, :, pl.ds(pl.multiple_of(yx * 128, 128), 128)]
                for col in range(4):
                    cs = slice(col * 512, (col + 1) * 512)
                    new = lax.dot_general(lhs, dh_ref[layer, :, cs], (((0,), (0,)), ((), ())), preferred_element_type=F32)
                    tot = (st_in[slot, :, cs] + new).astype(BF)
                    u_in[layer, yx // 2, lax.rem(yx, 2), 0, :, cs] = tot[:64]
                    u_in[layer, yx // 2, lax.rem(yx, 2), 1, :, cs] = tot[64:]

                @pl.when(n + 2 < 12)
                def _():
                    in_copy(n + 2).start()
                return carry
        else:
            def body(yx, carry):
                n = 4 * (layers - 1 - layer) + yx
                slot = lax.rem(n, 2)
                out_copy(n).wait()
                for part in range(4):
                    rows = pl.ds(part * 128, 128)
                    lhs = h_ref[layer, :, pl.ds(pl.multiple_of(yx * 512 + part * 128, 128), 128)]
                    new = lax.dot_general(lhs, g_ref[layer], (((0,), (0,)), ((), ())), preferred_element_type=F32)
                    tot = (st_out[slot, rows, :] + new).astype(BF)
                    u_out[layer, yx // 2, lax.rem(yx, 2), part // 2, pl.ds((part % 2) * 128, 128), :] = tot

                @pl.when(n + 2 < 12)
                def _():
                    out_copy(n + 2).start()
                return carry
        lax.fori_loop(0, 4, body, 0)

    def emb_produce(k):
        for half in range(2):
            n = 2 * k + half
            emb_copy(n, lambda cp: cp.wait())

            def body(q, carry):
                u_e[k, q // 2, lax.rem(q, 2), half] = st_e[n % 2, pl.ds(q, VOCAB_CHUNK, stride=4), :].astype(BF)
                return carry
            lax.fori_loop(0, 4, body, 0)
            if n + 2 < 2 * CHUNKS:
                emb_copy(n + 2, lambda cp: cp.start())

    def touched_produce():
        @pl.when(s > 0)
        def _():
            for step in range(stages):
                dx_send(step, 0).wait_recv()
        for half in range(2):
            hot = (slot_ref[half * 128:(half + 1) * 128, :] == ids_ref[...]).astype(F32).astype(BF)
            for q in range(4):
                new = jnp.dot(hot, dxb[:, q].reshape(128, 128), preferred_element_type=F32)
                u_t[q // 2, q % 2, half] = (touched_ref[pl.ds(half * 512 + q, 128, stride=4), :] + new).astype(BF)

    def unit_bufs(kind, i):
        if kind == 'e':
            return u_e.at[i], r0_e.at[i], r1_e.at[i], r2_e.at[i], VOCAB_CHUNK
        if kind == 't':
            return u_t, r0_t, r1_t, r2_t, 128
        if i % 2 == 0:
            return u_in.at[i // 2], r0_in.at[i // 2], r1_in.at[i // 2], r2_in.at[i // 2], 64
        return u_out.at[i // 2], r0_out.at[i // 2], r1_out.at[i // 2], r2_out.at[i // 2], 256

    def core_send(pos):
        u, r0, r1, r2, rows = unit_bufs(*UNIT_ORDER[pos])
        return send(u.at[:, :, 1 - c], r0, s0s.at[pos], s0r.at[pos], (s, core_peer))

    def first_send(pos):
        u, r0, r1, r2, rows = unit_bufs(*UNIT_ORDER[pos])
        if pos % 2 == 0:
            return send(u.at[:, 1 - x, c], r1, s1s.at[pos], s1r.at[pos], (s, x_peer))
        return send(u.at[1 - y, :, c], r1, s1s.at[pos], s1r.at[pos], (s, y_peer))

    def second_send(pos):
        u, r0, r1, r2, rows = unit_bufs(*UNIT_ORDER[pos])
        if pos % 2 == 0:
            return send(u.at[1 - y, x, c], r2, s2s.at[pos], s2r.at[pos], (s, y_peer))
        return send(u.at[y, 1 - x, c], r2, s2s.at[pos], s2r.at[pos], (s, x_peer))

    def stage_produce(pos):
        kind, i = UNIT_ORDER[pos]
        if kind == 'w':
            weight_produce(i)
        elif kind == 't':
            touched_produce()
        else:
            emb_produce(i)
        core_send(pos).start()

    def stage_add(pos):
        u, r0, r1, r2, rows = unit_bufs(*UNIT_ORDER[pos])
        core_send(pos).wait_recv()
        far = [(j, 1 - x) for j in range(2)] if pos % 2 == 0 else [(1 - y, j) for j in range(2)]
        near = [(j, x) for j in range(2)] if pos % 2 == 0 else [(y, j) for j in range(2)]
        for a, b in far:
            u[a, b, c] = u[a, b, c] + r0[a, b]
        first_send(pos).start()
        for a, b in near:
            u[a, b, c] = u[a, b, c] + r0[a, b]

    def stage_second(pos):
        u, r0, r1, r2, rows = unit_bufs(*UNIT_ORDER[pos])
        first_send(pos).wait_recv()
        far, i = ((1 - y, x), 1 - y) if pos % 2 == 0 else ((y, 1 - x), 1 - x)
        u[far[0], far[1], c] = u[far[0], far[1], c] + r1[i]
        second_send(pos).start()
        u[y, x, c] = u[y, x, c] + r1[1 - i]

    def piece(p, k):
        return agt.at[p] if k == TOUCH_GROUP else ag.at[p, pl.ds(*GROUPS[k])]

    def own_sends(k, act):
        for j, off in enumerate((1, -1) if k != TOUCH_GROUP else (1, -1, 2, -2, 3, -3)):
            @pl.when((s + off >= 0) & (s + off <= last))
            def _():
                blk = piece(2 * s + c, k)
                act(send(blk, blk, own_s.at[j, k], col_r.at[s, k], (jnp.clip(s + off, 0, last), d)))

    def far_send(k, hop, sign, act):
        z = s - sign * hop

        @pl.when((z >= 0) & (z <= last) & (s + sign >= 0) & (s + sign <= last))
        def _():
            zc = jnp.clip(z, 0, last)
            blk = piece(2 * zc + c, k)
            act(send(blk, blk, fwd_s.at[zc, k], col_r.at[zc, k], (jnp.clip(s + sign, 0, last), d)))

    def col_wait(z, k):
        blk = piece(2 * z + c, k)
        send(blk, blk, fwd_s.at[0, 0], col_r.at[z, k], (s, d)).wait_recv()

    def part_send(z, k):
        blk = piece(2 * z + c, k)
        return send(blk, blk, pt_s.at[z, k], pt_r.at[z, k], (s, core_peer))

    def emb_write(p, k):
        dst = patch_ref.at[p] if k == TOUCH_GROUP else emb_ref.at[p, pl.ds(*GROUPS[k])]
        return pltpu.make_async_copy(piece(p, k), dst, sem_t.at[p, k])

    def emit(p, k):
        emb_write(p, k).start()

    def have_piece(z, k):
        part_send(z, k).start()
        emit(2 * z + c, k)

    def stage_last(pos):
        kind, i = UNIT_ORDER[pos]
        u, r0, r1, r2, rows = unit_bufs(kind, i)
        second_send(pos).wait_recv()
        if kind == 'e':
            ag[2 * s + c, i] = u[y, x, c] + r2[...]
            for k, (first, count) in enumerate(GROUPS):
                if i == first + count - 1:
                    own_sends(k, lambda cp: cp.start())
                    have_piece(s, k)
        elif kind == 't':
            agt[2 * s + c] = u[y, x, c] + r2[...]
            own_sends(TOUCH_GROUP, lambda cp: cp.start())
            have_piece(s, TOUCH_GROUP)
        else:
            tot = (u[y, x, c].astype(F32) + r2[...].astype(F32))
            if i % 2 == 0:
                gin_ref[i // 2] = tot
            else:
                gout_ref[i // 2] = tot

    def part_event(z, k):
        part_send(z, k).wait_recv()
        emit(2 * z + 1 - c, k)

    def hop_event(k, hop):
        for sign in (-1, 1):
            z = s - sign * hop

            @pl.when((z >= 0) & (z <= last))
            def _():
                col_wait(jnp.clip(z, 0, last), k)
            if k != TOUCH_GROUP:
                far_send(k, hop, sign, lambda cp: cp.start())

            @pl.when((z >= 0) & (z <= last))
            def _():
                have_piece(jnp.clip(z, 0, last), k)

    events = [(k, hop) for hop in (1, 2, 3) for k in (0, 2, 1, 4, 3)]

    def run(slot):
        for op in slot.split():
            if op == 'h':
                hop_event(*events.pop(0))
            else:
                {'p': stage_produce, 'a': stage_add, 's': stage_second, 'l': stage_last}[op[0]](int(op[1:]))

    for k in range(stages):
        x_ref[0, k * rows:(k + 1) * rows, :] = stored_ref[jnp.maximum(last - s - k, 0)]
    pl.semaphore_wait(barrier, 3 + stages - 1)
    slots = list(CHAIN_SLOTS)
    run(slots.pop(0))
    for layer in range(layers):
        w_copies[2 * layer].wait()
        x_cur = x_ref[layer]
        for i in range(4):
            cs = slice(i * 512, (i + 1) * 512)
            pre = jnp.dot(x_cur, u_in[layer, :, :, :, :, cs].reshape(512, 512), preferred_element_type=F32).astype(BF)
            act, der = gelu_and_slope(pre.astype(F32))
            h_ref[layer, :, cs] = act.astype(BF)
            slope[layer, :, cs] = der
        run(slots.pop(0))
        w_copies[2 * layer + 1].wait()
        if layer < layers - 1:
            out = jnp.dot(h_ref[layer], u_out[layer].reshape(2048, 512), preferred_element_type=F32)
            x_ref[layer + 1] = (x_cur.astype(F32) + out).astype(BF)
        run(slots.pop(0))

    for k in range(stages):
        rs = slice(k * rows, (k + 1) * rows)
        active = s + k <= last
        for layer in range(layers - 1, -1, -1):
            @pl.when(active)
            def _():
                if layer < layers - 1:
                    cot = g_ref[layer, rs, :]
                else:
                    if k > 0:
                        cot_send(k - 1, s).wait_recv()
                        cot = cot_rcv[k - 1]
                    else:
                        cot = cot_ref[...]
                    g_ref[layer, rs, :] = cot
                back = cot.astype(F32)
                for i in range(4):
                    cs = slice(i * 512, (i + 1) * 512)
                    dh = lax.dot_general(cot, u_out[layer, i // 2, i % 2].reshape(512, 512), (((1,), (1,)), ((), ())), preferred_element_type=F32).astype(BF)
                    dh = (dh.astype(F32) * slope[layer, rs, cs]).astype(BF)
                    dh_ref[layer, rs, cs] = dh
                    back = back + lax.dot_general(dh, u_in[layer, :, :, :, :, cs].reshape(512, 512), (((1,), (1,)), ((), ())), preferred_element_type=F32)
                cot = back.astype(BF)
                if layer > 0:
                    g_ref[layer - 1, rs, :] = cot
                else:
                    cot_buf[k] = cot

                    @pl.when(s > 0)
                    def _():
                        cot_send(k, jnp.maximum(s - 1, 0)).start()

                    @pl.when(s == 0)
                    def _():
                        for q in range(4):
                            dxb[k, q] = cot[:, q * 128:(q + 1) * 128]
                        for z in range(1, stages):
                            dx_send(k, z).start()

            @pl.when(jnp.logical_not(active))
            def _():
                g_ref[layer, rs, :] = jnp.zeros((rows, 512), BF)
                dh_ref[layer, rs, :] = jnp.zeros((rows, 2048), BF)
            run(slots.pop(0))

    total = len(UNIT_ORDER)
    for slot in TAIL_SLOTS:
        run(slot)
    for hop in (1, 2, 3):
        hop_event(TOUCH_GROUP, hop)

    for k in range(TOUCH_GROUP + 1):
        for z in range(stages):
            part_event(z, k)

    for pos in range(total):
        core_send(pos).wait_send()
        first_send(pos).wait_send()
        second_send(pos).wait_send()

    for k in range(stages):
        @pl.when(s == 0)
        def _():
            for z in range(1, stages):
                dx_send(k, z).wait_send()

        @pl.when((s > 0) & (s + k <= last))
        def _():
            cot_send(k, jnp.maximum(s - 1, 0)).wait_send()

    def drain(z, k):
        part_send(z, k).wait_send()
        for core in range(2):
            emb_write(2 * z + core, k).wait()

    for k in range(TOUCH_GROUP + 1):
        for z in range(stages):
            drain(z, k)
    for k in range(TOUCH_GROUP + 1):
        own_sends(k, lambda cp: cp.wait_send())
        if k != TOUCH_GROUP:
            for hop in (1, 2):
                for sign in (-1, 1):
                    far_send(k, hop, sign, lambda cp: cp.wait_send())


def share_kernel(replicas, own_ref, all_ref, buf, send_sem, recv_sem):
    s = lax.axis_index('pp')
    d = lax.axis_index('dp')
    barrier = pltpu.get_barrier_semaphore()
    for off in range(1, replicas):
        pl.semaphore_signal(barrier, inc=1, device_id=(s, lax.rem(d + off, replicas)), device_id_type=MESH_ID)
    pl.semaphore_wait(barrier, replicas - 1)

    def copy(off):
        return pltpu.make_async_remote_copy(src_ref=own_ref, dst_ref=buf.at[d], send_sem=send_sem.at[off], recv_sem=recv_sem.at[d],
                                            device_id=(s, lax.rem(d + off, replicas)), device_id_type=MESH_ID)
    for off in range(1, replicas):
        copy(off).start()
    buf[d] = own_ref[...]
    for off in range(1, replicas):
        src = lax.rem(d + off, replicas)
        pltpu.make_async_remote_copy(src_ref=own_ref, dst_ref=buf.at[src], send_sem=send_sem.at[off], recv_sem=recv_sem.at[src],
                                     device_id=(s, src), device_id_type=MESH_ID).wait_recv()
    for off in range(1, replicas):
        copy(off).wait_send()
    all_ref[...] = buf[...]


def gather_kernel(ids_ref, emb_ref, out_ref, sem):
    replicas, _, tokens = ids_ref.shape
    z = lax.axis_index('pp')

    def body(i, carry):
        r, t = i // (tokens // 8), lax.rem(i, tokens // 8) * 8
        for j in range(8):
            pltpu.make_async_copy(emb_ref.at[ids_ref[r, z, t + j]], out_ref.at[i * 8 + j], sem).start()
        return carry
    lax.fori_loop(0, replicas * tokens // 8, body, 0)
    pltpu.make_async_copy(emb_ref.at[pl.ds(0, replicas * tokens)], out_ref, sem).wait()


def finish_kernel(scale, ids_ref, base_ref, patch_ref, gin_ref, gout_ref, emb_out, gin_out, gout_out, rows_f, patch_f, stage, sem):
    step = pl.program_id(0)
    core = lax.rem(lax.axis_index('dp'), 2)
    chunks = base_ref.shape[0]

    @pl.when(step == 0)
    def _():
        def copy(i):
            return pltpu.make_async_copy(base_ref.at[i], stage.at[i], sem.at[i])
        for i in range(chunks):
            copy(i).start()
        gin_out[...] = gin_ref[...] * scale
        gout_out[...] = gout_ref[...] * scale
        patch_f[...] = patch_ref[...].astype(F32)

        def widen(i, carry):
            copy(i).wait()
            rows_f[pl.ds(pl.multiple_of(i * VOCAB_CHUNK, VOCAB_CHUNK), VOCAB_CHUNK), :] = stage[i].astype(F32)
            return carry
        lax.fori_loop(0, chunks, widen, 0)

        replicas, stages, tokens = ids_ref.shape

        def put(i, carry):
            z, r, t = i // (replicas * tokens // 8), lax.rem(i // (tokens // 8), replicas), lax.rem(i, tokens // 8) * 8
            for j in range(8):
                rows_f[pl.ds(ids_ref[r, z, t + j], 1), :] = patch_f[pl.ds(i * 8 + j, 1), :]
            return carry
        lax.fori_loop(0, patch_f.shape[0] // 8, put, 0)

    pick = lax.broadcasted_iota(jnp.int32, (64, 128), 1) == lax.broadcasted_iota(jnp.int32, (64, 128), 0) + 64 * core
    sel = jnp.where(pick, scale, 0.0).astype(BF)
    for i in range(FINISH_BLOCK // VOCAB_CHUNK):
        start = pl.multiple_of(step * FINISH_BLOCK + i * VOCAB_CHUNK, VOCAB_CHUNK)
        block = rows_f[pl.ds(start, VOCAB_CHUNK), :].astype(BF)
        emb_out[:, i * VOCAB_CHUNK:(i + 1) * VOCAB_CHUNK] = lax.dot_general(sel, block, (((1,), (1,)), ((), ())), preferred_element_type=F32)


def solution(mesh):
    stages = mesh.shape['pp']
    replicas = mesh.shape['dp']

    def device_body(tok_ids, d_out, stored_x, w_in, w_out, acc_in, acc_out, acc_emb):
        layers, hid, ff = w_in.shape
        vocab = acc_emb.shape[1]
        tokens = d_out.shape[1]
        rows = tokens * stages
        steps_ids = tok_ids[::-1]
        ids = steps_ids.reshape(1, rows)
        vm = pl.BlockSpec(memory_space=pltpu.VMEM)
        hbm = pl.BlockSpec(memory_space=pltpu.HBM)
        smem = pl.BlockSpec(memory_space=pltpu.SMEM)
        dma = pltpu.SemaphoreType.DMA
        slot_ids = pl.pallas_call(
            functools.partial(share_kernel, replicas),
            out_shape=jax.ShapeDtypeStruct((replicas, stages, tokens), jnp.int32),
            in_specs=[vm], out_specs=vm,
            scratch_shapes=[pltpu.VMEM((replicas, stages, tokens), jnp.int32), dma((replicas,)), dma((replicas,))],
            compiler_params=pltpu.CompilerParams(collective_id=1, has_side_effects=True),
            name='share_ids',
        )(steps_ids)
        own_slots = lax.dynamic_index_in_dim(slot_ids, lax.axis_index('pp'), axis=1, keepdims=False)
        touched = pl.pallas_call(
            gather_kernel,
            out_shape=jax.ShapeDtypeStruct((replicas * tokens, 4, 128), F32),
            in_specs=[smem, hbm], out_specs=vm, scratch_shapes=[pltpu.SemaphoreType.DMA],
            name='gather_rows',
        )(slot_ids, acc_emb.reshape(vocab, 4, 128))
        v = pltpu.VMEM
        dma = pltpu.SemaphoreType.DMA
        units = len(UNIT_ORDER)
        gin, gout, emb, patch = pl.pallas_call(
            functools.partial(comm_kernel, stages, layers, vocab),
            out_shape=(jax.ShapeDtypeStruct((layers, hid // 8, ff), F32), jax.ShapeDtypeStruct((layers, ff // 8, hid), F32),
                       jax.ShapeDtypeStruct((2 * stages, CHUNKS, VOCAB_CHUNK, 128), BF), jax.ShapeDtypeStruct((2 * stages, 128, 128), BF)),
            in_specs=[vm] * 5 + [hbm] * 5,
            out_specs=(vm, vm, hbm, hbm),
            scratch_shapes=[
                v((layers, rows, hid), BF), v((layers, rows, ff), BF), v((layers, rows, hid), BF), v((layers, rows, ff), BF), v((layers, rows, ff), F32),
                v((stages, tokens, hid), BF), v((stages, tokens, hid), BF), dma((2 * layers,)), dma((stages,)), dma((stages,)),
                v((layers, 2, 2, 2, 64, ff), BF), v((layers, 2, 2, 64, ff), BF), v((layers, 2, 64, ff), BF), v((layers, 64, ff), BF),
                v((layers, 2, 2, 2, 256, hid), BF), v((layers, 2, 2, 256, hid), BF), v((layers, 2, 256, hid), BF), v((layers, 256, hid), BF),
                v((CHUNKS, 2, 2, 2, VOCAB_CHUNK, 128), BF), v((CHUNKS, 2, 2, VOCAB_CHUNK, 128), BF), v((CHUNKS, 2, VOCAB_CHUNK, 128), BF), v((CHUNKS, VOCAB_CHUNK, 128), BF),
                v((2, 2, 2, 128, 128), BF), v((2, 2, 128, 128), BF), v((2, 128, 128), BF), v((128, 128), BF),
                v((2 * stages, CHUNKS, VOCAB_CHUNK, 128), BF), v((2 * stages, 128, 128), BF), v((stages, 4, tokens, 128), BF),
                v((2, 128, ff), F32), v((2, 512, hid), F32), v((2, VOCAB_CHUNK * 4, 128), F32),
                dma((2,)), dma((2,)), dma((2,)), dma((2 * stages, CHUNKS + 1)),
                dma((units,)), dma((units,)), dma((units,)), dma((units,)), dma((units,)), dma((units,)),
                dma((stages, stages)), dma((stages,)), dma((6, CHUNKS + 1)), dma((stages, CHUNKS)), dma((stages, CHUNKS + 1)), dma((stages, CHUNKS + 1)), dma((stages, CHUNKS + 1)),
            ],
            compiler_params=pltpu.CompilerParams(collective_id=0, has_side_effects=True, vmem_limit_bytes=67043328),
            name='reduce_exchange',
        )(ids, own_slots.reshape(-1, 1), touched.reshape(-1, 128), d_out[0], stored_x[0], w_in.reshape(layers, 2, 2, 2, 64, ff), w_out.reshape(layers, 2, 2, 2, 256, hid), acc_in.reshape(layers, hid, ff), acc_out.reshape(layers, ff, hid), acc_emb.reshape(vocab * 4, 128))
        grad_emb, grad_in, grad_out = pl.pallas_call(
            functools.partial(finish_kernel, 1.0 / replicas),
            out_shape=(jax.ShapeDtypeStruct((64, vocab), F32), jax.ShapeDtypeStruct(gin.shape, F32), jax.ShapeDtypeStruct(gout.shape, F32)),
            grid=(2 * stages * HALF_VOCAB // FINISH_BLOCK,),
            in_specs=[smem, hbm, vm, vm, vm],
            out_specs=(pl.BlockSpec((64, FINISH_BLOCK), lambda i: (0, i)), vm, vm),
            scratch_shapes=[v((2 * stages * CHUNKS * VOCAB_CHUNK, 128), F32), v((stages * replicas * tokens, 128), F32),
                            v((2 * stages * CHUNKS, VOCAB_CHUNK, 128), BF), dma((2 * stages * CHUNKS,))],
            compiler_params=pltpu.CompilerParams(vmem_limit_bytes=58 * 2 ** 20, dimension_semantics=('arbitrary',)),
            name='finish',
        )(slot_ids, emb.reshape(2 * stages * CHUNKS, VOCAB_CHUNK, 128), patch.reshape(-1, 128), gin, gout)
        return grad_in, grad_out, grad_emb.T

    return jax.shard_map(device_body, mesh=mesh, in_specs=(P(None, 'dp'), P('pp', 'dp', None), P('pp', None, 'dp', None), P('pp', None, None), P('pp', None, None), P('pp', 'dp', None, None), P('pp', 'dp', None, None), P('dp', None, None)), out_specs=(P('pp', 'dp', None), P('pp', 'dp', None), P(None, 'dp')), check_vma=False)
```

```python
import functools

import jax
import jax.numpy as jnp
from jax import lax
from jax.experimental import pallas as pl
from jax.experimental.pallas import tpu as pltpu
from jax.sharding import PartitionSpec as P

MESH_ID = pl.DeviceIdType.MESH
BF = jnp.bfloat16
F32 = jnp.float32

VOCAB_CHUNK = 768
CHUNKS = 5
HALF_VOCAB = VOCAB_CHUNK * CHUNKS
WEIGHT_UNITS = 6
FINISH_BLOCK = 3072
UNIT_ORDER = tuple(('e', i) for i in range(CHUNKS)) + (('w', 5), ('w', 4), ('t', 0), ('w', 3), ('w', 2), ('w', 1), ('w', 0))
GROUPS = ((0, 1), (1, 1), (2, 1), (3, 1), (4, 1))
TOUCH_GROUP = len(GROUPS)
CHAIN_SLOTS = (
    ('p0',),
    ('p1',),
    ('a0', 'p2'),
    ('a1', 'p3'),
    ('a2', 'p4'),
    (),
    (),
    (),
    (),
    ('s0', 'a3', 's1', 'a4'),
    (),
    (),
    ('l0', 's2'),
    ('l1',),
    (),
    ('s3', 'h'),
    ('s4', 'l2', 'p5', 'h', 'p6'),
    ('a5', 'l3'),
    ('a6', 'l4', 'h', 'p7', 'p8', 'a7'),
)
TAIL_SLOTS = (
    ('p9', 'p10', 'h', 'a8', 'p11', 'h', 'a9', 's5', 's7', 'h', 's6'),
    ('a11', 'a10', 'h', 'h', 's9', 's8', 'h'),
    ('l6', 'l5', 'l7', 'h'),
    ('s11', 's10', 'h', 'h', 'h'),
    ('l8', 'l9', 'h'),
    ('l10', 'h'),
    ('l11',),
)


def gelu_and_slope(pre):
    return jax.jvp(jax.nn.gelu, (pre,), (jnp.ones_like(pre),))


def comm_kernel(stages, layers, vocab, ids_ref, slot_ref, touched_ref, cot_ref, stored_ref, w_in, w_out, acc_in, acc_out, acc_emb,
                gin_ref, gout_ref, emb_ref, patch_ref, x_ref, h_ref, g_ref, dh_ref, slope, cot_buf, cot_rcv,
                sem_w, sem_cs, sem_cr,
                u_in, r0_in, r1_in, r2_in, u_out, r0_out, r1_out, r2_out, u_e, r0_e, r1_e, r2_e, u_t, r0_t, r1_t, r2_t,
                ag, agt, dxb, st_in, st_out, st_e,
                sem_st_in, sem_st_out, sem_st_e, sem_t, s0s, s0r, s1s, s1r, s2s, s2r,
                dxs, dxr, own_s, fwd_s, pt_s, col_r, pt_r):
    s = lax.axis_index('pp')
    d = lax.axis_index('dp')
    c = lax.rem(d, 2)
    x = lax.rem(d // 2, 2)
    y = d // 4
    core_peer = d + 1 - 2 * c
    x_peer = d + 2 - 4 * x
    y_peer = d + 4 - 8 * y
    last = stages - 1

    def send(src, dst, ss, rs, target):
        return pltpu.make_async_remote_copy(src_ref=src, dst_ref=dst, send_sem=ss, recv_sem=rs, device_id=target, device_id_type=MESH_ID)

    barrier = pltpu.get_barrier_semaphore()
    for peer in (core_peer, x_peer, y_peer):
        pl.semaphore_signal(barrier, inc=1, device_id=(s, peer), device_id_type=MESH_ID)
    for off in range(1, stages):
        pl.semaphore_signal(barrier, inc=1, device_id=(lax.rem(s + off, stages), d), device_id_type=MESH_ID)

    def in_copy(n):
        unit, yx = n // 4, lax.rem(n, 4)
        slot = lax.rem(n, 2)
        return pltpu.make_async_copy(acc_in.at[layers - 1 - unit, pl.ds(yx * 128, 128), :], st_in.at[slot], sem_st_in.at[slot])

    def out_copy(n):
        unit, yx = n // 4, lax.rem(n, 4)
        slot = lax.rem(n, 2)
        return pltpu.make_async_copy(acc_out.at[layers - 1 - unit, pl.ds(yx * 512, 512), :], st_out.at[slot], sem_st_out.at[slot])

    part_rows = HALF_VOCAB * 4
    chunk_rows = VOCAB_CHUNK * 4
    tail_rows = vocab * 4 - (part_rows * 2 * stages - chunk_rows)

    def emb_copy(n, act):
        k, half = n // 2, n % 2
        slot = n % 2
        start = pl.multiple_of(s * (2 * part_rows) + half * part_rows + k * chunk_rows, 8)

        def full():
            act(pltpu.make_async_copy(acc_emb.at[pl.ds(start, chunk_rows), :], st_e.at[slot], sem_st_e.at[slot]))

        if k == CHUNKS - 1 and half == 1:
            @pl.when(s == last)
            def _():
                act(pltpu.make_async_copy(acc_emb.at[pl.ds(vocab * 4 - tail_rows, tail_rows), :],
                                          st_e.at[slot, pl.ds(0, tail_rows), :], sem_st_e.at[slot]))

            @pl.when(s != last)
            def _():
                full()
        else:
            full()

    w_copies = []
    for layer in range(layers):
        for j, (w, u) in enumerate(((w_in, u_in), (w_out, u_out))):
            w_copies.append(pltpu.make_async_copy(w.at[layer], u.at[layer], sem_w.at[2 * layer + j]))
            w_copies[-1].start()
    for n in range(2):
        in_copy(jnp.int32(n)).start()
        out_copy(jnp.int32(n)).start()
        emb_copy(n, lambda cp: cp.start())

    rows = cot_ref.shape[0]

    def dx_send(k, z):
        return send(dxb.at[k], dxb.at[k], dxs.at[k, z], dxr.at[k], (z, d))

    def cot_send(k, target):
        return send(cot_buf.at[k], cot_rcv.at[k], sem_cs.at[k], sem_cr.at[k], (target, d))

    def weight_produce(unit):
        layer = unit // 2
        if unit % 2 == 0:
            def body(yx, carry):
                n = 4 * (layers - 1 - layer) + yx
                slot = lax.rem(n, 2)
                in_copy(n).wait()
                lhs = x_ref[layer, :, pl.ds(pl.multiple_of(yx * 128, 128), 128)]
                for col in range(4):
                    cs = slice(col * 512, (col + 1) * 512)
                    new = lax.dot_general(lhs, dh_ref[layer, :, cs], (((0,), (0,)), ((), ())), preferred_element_type=F32)
                    tot = (st_in[slot, :, cs] + new).astype(BF)
                    u_in[layer, yx // 2, lax.rem(yx, 2), 0, :, cs] = tot[:64]
                    u_in[layer, yx // 2, lax.rem(yx, 2), 1, :, cs] = tot[64:]

                @pl.when(n + 2 < 12)
                def _():
                    in_copy(n + 2).start()
                return carry
        else:
            def body(yx, carry):
                n = 4 * (layers - 1 - layer) + yx
                slot = lax.rem(n, 2)
                out_copy(n).wait()
                for part in range(4):
                    rows = pl.ds(part * 128, 128)
                    lhs = h_ref[layer, :, pl.ds(pl.multiple_of(yx * 512 + part * 128, 128), 128)]
                    new = lax.dot_general(lhs, g_ref[layer], (((0,), (0,)), ((), ())), preferred_element_type=F32)
                    tot = (st_out[slot, rows, :] + new).astype(BF)
                    u_out[layer, yx // 2, lax.rem(yx, 2), part // 2, pl.ds((part % 2) * 128, 128), :] = tot

                @pl.when(n + 2 < 12)
                def _():
                    out_copy(n + 2).start()
                return carry
        lax.fori_loop(0, 4, body, 0)

    def emb_produce(k):
        for half in range(2):
            n = 2 * k + half
            emb_copy(n, lambda cp: cp.wait())

            def body(q, carry):
                u_e[k, q // 2, lax.rem(q, 2), half] = st_e[n % 2, pl.ds(q, VOCAB_CHUNK, stride=4), :].astype(BF)
                return carry
            lax.fori_loop(0, 4, body, 0)
            if n + 2 < 2 * CHUNKS:
                emb_copy(n + 2, lambda cp: cp.start())

    def touched_produce():
        @pl.when(s > 0)
        def _():
            for step in range(stages):
                dx_send(step, 0).wait_recv()
        for r in range(8):
            hot = (ids_ref[...] == slot_ref[r, pl.ds(last - s, 1), :]).astype(F32).astype(BF)
            for q in range(4):
                new = lax.dot_general(hot, dxb[:, q].reshape(128, 128), (((0,), (0,)), ((), ())), preferred_element_type=F32)
                old = touched_ref[pl.ds(r * 128 + q, 32, stride=4), :]
                u_t[q // 2, q % 2, r // 4, (r % 4) * 32:(r % 4 + 1) * 32, :] = (old + new).astype(BF)

    def unit_bufs(kind, i):
        if kind == 'e':
            return u_e.at[i], r0_e.at[i], r1_e.at[i], r2_e.at[i], VOCAB_CHUNK
        if kind == 't':
            return u_t, r0_t, r1_t, r2_t, 128
        if i % 2 == 0:
            return u_in.at[i // 2], r0_in.at[i // 2], r1_in.at[i // 2], r2_in.at[i // 2], 64
        return u_out.at[i // 2], r0_out.at[i // 2], r1_out.at[i // 2], r2_out.at[i // 2], 256

    def core_send(pos):
        u, r0, r1, r2, rows = unit_bufs(*UNIT_ORDER[pos])
        return send(u.at[:, :, 1 - c], r0, s0s.at[pos], s0r.at[pos], (s, core_peer))

    def first_send(pos):
        u, r0, r1, r2, rows = unit_bufs(*UNIT_ORDER[pos])
        if pos % 2 == 0:
            return send(u.at[:, 1 - x, c], r1, s1s.at[pos], s1r.at[pos], (s, x_peer))
        return send(u.at[1 - y, :, c], r1, s1s.at[pos], s1r.at[pos], (s, y_peer))

    def second_send(pos):
        u, r0, r1, r2, rows = unit_bufs(*UNIT_ORDER[pos])
        if pos % 2 == 0:
            return send(u.at[1 - y, x, c], r2, s2s.at[pos], s2r.at[pos], (s, y_peer))
        return send(u.at[y, 1 - x, c], r2, s2s.at[pos], s2r.at[pos], (s, x_peer))

    def stage_produce(pos):
        kind, i = UNIT_ORDER[pos]
        if kind == 'w':
            weight_produce(i)
        elif kind == 't':
            touched_produce()
        else:
            emb_produce(i)
        core_send(pos).start()

    def stage_add(pos):
        u, r0, r1, r2, rows = unit_bufs(*UNIT_ORDER[pos])
        core_send(pos).wait_recv()
        far = [(j, 1 - x) for j in range(2)] if pos % 2 == 0 else [(1 - y, j) for j in range(2)]
        near = [(j, x) for j in range(2)] if pos % 2 == 0 else [(y, j) for j in range(2)]
        for a, b in far:
            u[a, b, c] = u[a, b, c] + r0[a, b]
        first_send(pos).start()
        for a, b in near:
            u[a, b, c] = u[a, b, c] + r0[a, b]

    def stage_second(pos):
        u, r0, r1, r2, rows = unit_bufs(*UNIT_ORDER[pos])
        first_send(pos).wait_recv()
        far, i = ((1 - y, x), 1 - y) if pos % 2 == 0 else ((y, 1 - x), 1 - x)
        u[far[0], far[1], c] = u[far[0], far[1], c] + r1[i]
        second_send(pos).start()
        u[y, x, c] = u[y, x, c] + r1[1 - i]

    def piece(p, k):
        return agt.at[p] if k == TOUCH_GROUP else ag.at[p, pl.ds(*GROUPS[k])]

    def own_sends(k, act):
        for j, off in enumerate((1, -1) if k != TOUCH_GROUP else (1, -1, 2, -2, 3, -3)):
            @pl.when((s + off >= 0) & (s + off <= last))
            def _():
                blk = piece(2 * s + c, k)
                act(send(blk, blk, own_s.at[j, k], col_r.at[s, k], (jnp.clip(s + off, 0, last), d)))

    def far_send(k, hop, sign, act):
        z = s - sign * hop

        @pl.when((z >= 0) & (z <= last) & (s + sign >= 0) & (s + sign <= last))
        def _():
            zc = jnp.clip(z, 0, last)
            blk = piece(2 * zc + c, k)
            act(send(blk, blk, fwd_s.at[zc, k], col_r.at[zc, k], (jnp.clip(s + sign, 0, last), d)))

    def col_wait(z, k):
        blk = piece(2 * z + c, k)
        send(blk, blk, fwd_s.at[0, 0], col_r.at[z, k], (s, d)).wait_recv()

    def part_send(z, k):
        blk = piece(2 * z + c, k)
        return send(blk, blk, pt_s.at[z, k], pt_r.at[z, k], (s, core_peer))

    def emb_write(p, k):
        dst = patch_ref.at[p] if k == TOUCH_GROUP else emb_ref.at[p, pl.ds(*GROUPS[k])]
        return pltpu.make_async_copy(piece(p, k), dst, sem_t.at[p, k])

    def emit(p, k):
        emb_write(p, k).start()

    def have_piece(z, k):
        part_send(z, k).start()
        emit(2 * z + c, k)

    def stage_last(pos):
        kind, i = UNIT_ORDER[pos]
        u, r0, r1, r2, rows = unit_bufs(kind, i)
        second_send(pos).wait_recv()
        if kind == 'e':
            ag[2 * s + c, i] = u[y, x, c] + r2[...]
            for k, (first, count) in enumerate(GROUPS):
                if i == first + count - 1:
                    own_sends(k, lambda cp: cp.start())
                    have_piece(s, k)
        elif kind == 't':
            agt[2 * s + c] = u[y, x, c] + r2[...]
            own_sends(TOUCH_GROUP, lambda cp: cp.start())
            have_piece(s, TOUCH_GROUP)
        else:
            tot = (u[y, x, c].astype(F32) + r2[...].astype(F32))
            if i % 2 == 0:
                gin_ref[i // 2] = tot
            else:
                gout_ref[i // 2] = tot

    def part_event(z, k):
        part_send(z, k).wait_recv()
        emit(2 * z + 1 - c, k)

    def hop_event(k, hop):
        for sign in (-1, 1):
            z = s - sign * hop

            @pl.when((z >= 0) & (z <= last))
            def _():
                col_wait(jnp.clip(z, 0, last), k)
            if k != TOUCH_GROUP:
                far_send(k, hop, sign, lambda cp: cp.start())

            @pl.when((z >= 0) & (z <= last))
            def _():
                have_piece(jnp.clip(z, 0, last), k)

    events = [(k, hop) for hop in (1, 2, 3) for k in range(TOUCH_GROUP)]

    def run(slot):
        for op in slot:
            if op == 'h':
                hop_event(*events.pop(0))
            else:
                {'p': stage_produce, 'a': stage_add, 's': stage_second, 'l': stage_last}[op[0]](int(op[1:]))

    for k in range(stages):
        x_ref[0, k * rows:(k + 1) * rows, :] = stored_ref[jnp.maximum(last - s - k, 0)]
    pl.semaphore_wait(barrier, 3 + stages - 1)
    slots = list(CHAIN_SLOTS)
    run(slots.pop(0))
    for layer in range(layers):
        w_copies[2 * layer].wait()
        x_cur = x_ref[layer]
        for i in range(4):
            cs = slice(i * 512, (i + 1) * 512)
            pre = jnp.dot(x_cur, u_in[layer, :, :, :, :, cs].reshape(512, 512), preferred_element_type=F32).astype(BF)
            act, der = gelu_and_slope(pre.astype(F32))
            h_ref[layer, :, cs] = act.astype(BF)
            slope[layer, :, cs] = der
        run(slots.pop(0))
        w_copies[2 * layer + 1].wait()
        if layer < layers - 1:
            out = jnp.dot(h_ref[layer], u_out[layer].reshape(2048, 512), preferred_element_type=F32)
            x_ref[layer + 1] = (x_cur.astype(F32) + out).astype(BF)
        run(slots.pop(0))

    for k in range(stages):
        rs = slice(k * rows, (k + 1) * rows)
        active = s + k <= last
        for layer in range(layers - 1, -1, -1):
            @pl.when(active)
            def _():
                if layer < layers - 1:
                    cot = g_ref[layer, rs, :]
                else:
                    if k > 0:
                        cot_send(k - 1, s).wait_recv()
                        cot = cot_rcv[k - 1]
                    else:
                        cot = cot_ref[...]
                    g_ref[layer, rs, :] = cot
                back = cot.astype(F32)
                for i in range(4):
                    cs = slice(i * 512, (i + 1) * 512)
                    dh = lax.dot_general(cot, u_out[layer, i // 2, i % 2].reshape(512, 512), (((1,), (1,)), ((), ())), preferred_element_type=F32).astype(BF)
                    dh = (dh.astype(F32) * slope[layer, rs, cs]).astype(BF)
                    dh_ref[layer, rs, cs] = dh
                    back = back + lax.dot_general(dh, u_in[layer, :, :, :, :, cs].reshape(512, 512), (((1,), (1,)), ((), ())), preferred_element_type=F32)
                cot = back.astype(BF)
                if layer > 0:
                    g_ref[layer - 1, rs, :] = cot
                else:
                    cot_buf[k] = cot

                    @pl.when(s > 0)
                    def _():
                        cot_send(k, jnp.maximum(s - 1, 0)).start()

                    @pl.when(s == 0)
                    def _():
                        for q in range(4):
                            dxb[k, q] = cot[:, q * 128:(q + 1) * 128]
                        for z in range(1, stages):
                            dx_send(k, z).start()

            @pl.when(jnp.logical_not(active))
            def _():
                g_ref[layer, rs, :] = jnp.zeros((rows, 512), BF)
                dh_ref[layer, rs, :] = jnp.zeros((rows, 2048), BF)
            run(slots.pop(0))

    total = len(UNIT_ORDER)
    for slot in TAIL_SLOTS:
        run(slot)
    for hop in (1, 2, 3):
        hop_event(TOUCH_GROUP, hop)

    for k in range(TOUCH_GROUP + 1):
        for z in range(stages):
            part_event(z, k)

    for pos in range(total):
        core_send(pos).wait_send()
        first_send(pos).wait_send()
        second_send(pos).wait_send()

    for k in range(stages):
        @pl.when(s == 0)
        def _():
            for z in range(1, stages):
                dx_send(k, z).wait_send()

        @pl.when((s > 0) & (s + k <= last))
        def _():
            cot_send(k, jnp.maximum(s - 1, 0)).wait_send()

    def drain(z, k):
        part_send(z, k).wait_send()
        for core in range(2):
            emb_write(2 * z + core, k).wait()

    for k in range(TOUCH_GROUP + 1):
        for z in range(stages):
            drain(z, k)
    for k in range(TOUCH_GROUP + 1):
        own_sends(k, lambda cp: cp.wait_send())
        if k != TOUCH_GROUP:
            for hop in (1, 2):
                for sign in (-1, 1):
                    far_send(k, hop, sign, lambda cp: cp.wait_send())


def share_kernel(replicas, own_ref, all_ref, buf, send_sem, recv_sem):
    s = lax.axis_index('pp')
    d = lax.axis_index('dp')
    barrier = pltpu.get_barrier_semaphore()
    for off in range(1, replicas):
        pl.semaphore_signal(barrier, inc=1, device_id=(s, lax.rem(d + off, replicas)), device_id_type=MESH_ID)
    pl.semaphore_wait(barrier, replicas - 1)

    def copy(off):
        return pltpu.make_async_remote_copy(src_ref=own_ref, dst_ref=buf.at[d], send_sem=send_sem.at[off], recv_sem=recv_sem.at[d],
                                            device_id=(s, lax.rem(d + off, replicas)), device_id_type=MESH_ID)
    for off in range(1, replicas):
        copy(off).start()
    buf[d] = own_ref[...]
    for off in range(1, replicas):
        src = lax.rem(d + off, replicas)
        pltpu.make_async_remote_copy(src_ref=own_ref, dst_ref=buf.at[src], send_sem=send_sem.at[off], recv_sem=recv_sem.at[src],
                                     device_id=(s, src), device_id_type=MESH_ID).wait_recv()
    for off in range(1, replicas):
        copy(off).wait_send()
    all_ref[...] = buf[...]


def gather_kernel(ids_ref, emb_ref, out_ref, sem):
    replicas, _, tokens = ids_ref.shape
    z = ids_ref.shape[1] - 1 - lax.axis_index('pp')

    def body(i, carry):
        r, t = i // (tokens // 8), lax.rem(i, tokens // 8) * 8
        for j in range(8):
            pltpu.make_async_copy(emb_ref.at[ids_ref[r, z, t + j]], out_ref.at[i * 8 + j], sem).start()
        return carry
    lax.fori_loop(0, replicas * tokens // 8, body, 0)
    pltpu.make_async_copy(emb_ref.at[pl.ds(0, replicas * tokens)], out_ref, sem).wait()


def finish_kernel(scale, ids_ref, base_ref, patch_ref, gin_ref, gout_ref, emb_out, gin_out, gout_out, rows_f, patch_f, stage, sem):
    step = pl.program_id(0)
    core = lax.rem(lax.axis_index('dp'), 2)
    chunks = base_ref.shape[0]

    @pl.when(step == 0)
    def _():
        def copy(i):
            return pltpu.make_async_copy(base_ref.at[i], stage.at[pl.ds(pl.multiple_of(i * VOCAB_CHUNK, VOCAB_CHUNK), VOCAB_CHUNK), :], sem.at[i])
        for i in range(chunks):
            copy(i).start()
        gin_out[...] = gin_ref[...] * scale
        gout_out[...] = gout_ref[...] * scale
        patch_f[...] = patch_ref[...].astype(F32)

        def widen(i, carry):
            copy(i).wait()
            chunk = pl.ds(pl.multiple_of(i * VOCAB_CHUNK, VOCAB_CHUNK), VOCAB_CHUNK)
            rows_f[chunk, :] = stage[chunk, :].astype(F32)
            return carry
        lax.fori_loop(0, chunks, widen, 0)

        replicas, stages, tokens = ids_ref.shape

        def put(i, carry):
            z, r, t = i // (replicas * tokens // 8), lax.rem(i // (tokens // 8), replicas), lax.rem(i, tokens // 8) * 8
            for j in range(8):
                rows_f[pl.ds(ids_ref[r, stages - 1 - z, t + j], 1), :] = patch_f[pl.ds(i * 8 + j, 1), :]
            return carry
        lax.fori_loop(0, patch_f.shape[0] // 8, put, 0)

    pick = lax.broadcasted_iota(jnp.int32, (64, 128), 1) == lax.broadcasted_iota(jnp.int32, (64, 128), 0) + 64 * core
    sel = jnp.where(pick, scale, 0.0).astype(BF)
    for i in range(FINISH_BLOCK // VOCAB_CHUNK):
        start = pl.multiple_of(step * FINISH_BLOCK + i * VOCAB_CHUNK, VOCAB_CHUNK)
        block = rows_f[pl.ds(start, VOCAB_CHUNK), :].astype(BF)
        emb_out[:, i * VOCAB_CHUNK:(i + 1) * VOCAB_CHUNK] = lax.dot_general(sel, block, (((1,), (1,)), ((), ())), preferred_element_type=F32)


def solution(mesh):
    stages = mesh.shape['pp']
    replicas = mesh.shape['dp']

    def device_body(tok_ids, d_out, stored_x, w_in, w_out, acc_in, acc_out, acc_emb):
        layers, hid, ff = w_in.shape
        vocab = acc_emb.shape[1]
        tokens = d_out.shape[1]
        rows = tokens * stages
        ids = tok_ids[::-1].reshape(rows, 1)
        vm = pl.BlockSpec(memory_space=pltpu.VMEM)
        hbm = pl.BlockSpec(memory_space=pltpu.HBM)
        smem = pl.BlockSpec(memory_space=pltpu.SMEM)
        dma = pltpu.SemaphoreType.DMA
        slot_ids = pl.pallas_call(
            functools.partial(share_kernel, replicas),
            out_shape=jax.ShapeDtypeStruct((replicas, stages, tokens), jnp.int32),
            in_specs=[vm], out_specs=vm,
            scratch_shapes=[pltpu.VMEM((replicas, stages, tokens), jnp.int32), dma((replicas,)), dma((replicas,))],
            compiler_params=pltpu.CompilerParams(collective_id=1, has_side_effects=True),
            name='share_ids',
        )(tok_ids)
        touched = pl.pallas_call(
            gather_kernel,
            out_shape=jax.ShapeDtypeStruct((replicas * tokens, 4, 128), F32),
            in_specs=[smem, hbm], out_specs=vm, scratch_shapes=[pltpu.SemaphoreType.DMA],
            name='gather_rows',
        )(slot_ids, acc_emb.reshape(vocab, 4, 128))
        v = pltpu.VMEM
        dma = pltpu.SemaphoreType.DMA
        units = len(UNIT_ORDER)
        gin, gout, emb, patch = pl.pallas_call(
            functools.partial(comm_kernel, stages, layers, vocab),
            out_shape=(jax.ShapeDtypeStruct((layers, hid // 8, ff), F32), jax.ShapeDtypeStruct((layers, ff // 8, hid), F32),
                       jax.ShapeDtypeStruct((2 * stages, CHUNKS, VOCAB_CHUNK, 128), BF), jax.ShapeDtypeStruct((2 * stages, 128, 128), BF)),
            in_specs=[vm] * 5 + [hbm] * 5,
            out_specs=(vm, vm, hbm, hbm),
            scratch_shapes=[
                v((layers, rows, hid), BF), v((layers, rows, ff), BF), v((layers, rows, hid), BF), v((layers, rows, ff), BF), v((layers, rows, ff), F32),
                v((stages, tokens, hid), BF), v((stages, tokens, hid), BF), dma((2 * layers,)), dma((stages,)), dma((stages,)),
                v((layers, 2, 2, 2, 64, ff), BF), v((layers, 2, 2, 64, ff), BF), v((layers, 2, 64, ff), BF), v((layers, 64, ff), BF),
                v((layers, 2, 2, 2, 256, hid), BF), v((layers, 2, 2, 256, hid), BF), v((layers, 2, 256, hid), BF), v((layers, 256, hid), BF),
                v((CHUNKS, 2, 2, 2, VOCAB_CHUNK, 128), BF), v((CHUNKS, 2, 2, VOCAB_CHUNK, 128), BF), v((CHUNKS, 2, VOCAB_CHUNK, 128), BF), v((CHUNKS, VOCAB_CHUNK, 128), BF),
                v((2, 2, 2, 128, 128), BF), v((2, 2, 128, 128), BF), v((2, 128, 128), BF), v((128, 128), BF),
                v((2 * stages, CHUNKS, VOCAB_CHUNK, 128), BF), v((2 * stages, 128, 128), BF), v((stages, 4, tokens, 128), BF),
                v((2, 128, ff), F32), v((2, 512, hid), F32), v((2, VOCAB_CHUNK * 4, 128), F32),
                dma((2,)), dma((2,)), dma((2,)), dma((2 * stages, CHUNKS + 1)),
                dma((units,)), dma((units,)), dma((units,)), dma((units,)), dma((units,)), dma((units,)),
                dma((stages, stages)), dma((stages,)), dma((6, CHUNKS + 1)), dma((stages, CHUNKS)), dma((stages, CHUNKS + 1)), dma((stages, CHUNKS + 1)), dma((stages, CHUNKS + 1)),
            ],
            compiler_params=pltpu.CompilerParams(collective_id=0, has_side_effects=True, vmem_limit_bytes=67043328),
            name='reduce_exchange',
        )(ids, slot_ids, touched.reshape(-1, 128), d_out[0], stored_x[0], w_in.reshape(layers, 2, 2, 2, 64, ff), w_out.reshape(layers, 2, 2, 2, 256, hid), acc_in.reshape(layers, hid, ff), acc_out.reshape(layers, ff, hid), acc_emb.reshape(vocab * 4, 128))
        grad_emb, grad_in, grad_out = pl.pallas_call(
            functools.partial(finish_kernel, 1.0 / replicas),
            out_shape=(jax.ShapeDtypeStruct((64, vocab), F32), jax.ShapeDtypeStruct(gin.shape, F32), jax.ShapeDtypeStruct(gout.shape, F32)),
            grid=(2 * stages * HALF_VOCAB // FINISH_BLOCK,),
            in_specs=[smem, hbm, vm, vm, vm],
            out_specs=(pl.BlockSpec((64, FINISH_BLOCK), lambda i: (0, i)), vm, vm),
            scratch_shapes=[v((2 * stages * CHUNKS * VOCAB_CHUNK, 128), F32), v((stages * replicas * tokens, 128), F32),
                            v((2 * stages * CHUNKS * VOCAB_CHUNK, 128), BF), dma((2 * stages * CHUNKS,))],
            compiler_params=pltpu.CompilerParams(vmem_limit_bytes=58 * 2 ** 20, dimension_semantics=('arbitrary',)),
            name='finish',
        )(slot_ids, emb.reshape(2 * stages * CHUNKS, VOCAB_CHUNK, 128), patch.reshape(-1, 128), gin, gout)
        return grad_in, grad_out, grad_emb.T

    return jax.shard_map(device_body, mesh=mesh, in_specs=(P(None, 'dp'), P('pp', 'dp', None), P('pp', None, 'dp', None), P('pp', None, None), P('pp', None, None), P('pp', 'dp', None, None), P('pp', 'dp', None, None), P('dp', None, None)), out_specs=(P('pp', 'dp', None), P('pp', 'dp', None), P(None, 'dp')), check_vma=False)
```

```python
import functools

import jax
import jax.numpy as jnp
from jax import lax
from jax.experimental import pallas as pl
from jax.experimental.pallas import tpu as pltpu
from jax.sharding import PartitionSpec as P

MESH_ID = pl.DeviceIdType.MESH
BF = jnp.bfloat16
F32 = jnp.float32

VOCAB_CHUNK = 768
CHUNKS = 5
HALF_VOCAB = VOCAB_CHUNK * CHUNKS
WEIGHT_UNITS = 6
FINISH_BLOCK = 6144
UNIT_ORDER = tuple(('e', i) for i in range(CHUNKS)) + (('w', 5), ('w', 4), ('t', 0), ('w', 3), ('w', 2), ('w', 1), ('w', 0))
GROUPS = ((0, 1), (1, 1), (2, 1), (3, 1), (4, 1))
TOUCH_GROUP = len(GROUPS)
CHAIN_SLOTS = (
    ('p0',),
    ('p1',),
    ('a0', 'p2'),
    ('a1', 'p3'),
    ('a2', 'p4'),
    (),
    (),
    (),
    (),
    ('s0', 'a3', 's1', 'a4'),
    (),
    (),
    ('l0', 's2'),
    ('l1',),
    (),
    ('s3', 'h'),
    ('s4', 'l2', 'p5', 'h', 'p6'),
    ('a5', 'l3'),
    ('a6', 'l4', 'h', 'p7', 'p8', 'a7'),
)
TAIL_SLOTS = (
    ('p9', 'p10', 'h', 'a8', 'p11', 'h', 'a9', 's5', 's7', 'h', 's6'),
    ('a11', 'a10', 'h', 'h', 's9', 's8', 'h'),
    ('l6', 'l5', 'l7', 'h'),
    ('s11', 's10', 'h', 'h', 'h'),
    ('l8', 'l9', 'h'),
    ('l10', 'h'),
    ('l11',),
)


def gelu_and_slope(pre):
    return jax.jvp(jax.nn.gelu, (pre,), (jnp.ones_like(pre),))


def comm_kernel(stages, layers, vocab, ids_ref, slot_ref, touched_ref, cot_ref, stored_ref, w_in, w_out, acc_in, acc_out, acc_emb,
                gin_ref, gout_ref, emb_ref, patch_ref, x_ref, h_ref, g_ref, dh_ref, slope, cot_buf, cot_rcv,
                sem_w, sem_cs, sem_cr,
                u_in, r0_in, r1_in, r2_in, u_out, r0_out, r1_out, r2_out, u_e, r0_e, r1_e, r2_e, u_t, r0_t, r1_t, r2_t,
                ag, agt, dxb, st_in, st_out, st_e,
                sem_st_in, sem_st_out, sem_st_e, sem_t, s0s, s0r, s1s, s1r, s2s, s2r,
                dxs, dxr, own_s, fwd_s, pt_s, col_r, pt_r):
    s = lax.axis_index('pp')
    d = lax.axis_index('dp')
    c = lax.rem(d, 2)
    x = lax.rem(d // 2, 2)
    y = d // 4
    core_peer = d + 1 - 2 * c
    x_peer = d + 2 - 4 * x
    y_peer = d + 4 - 8 * y
    last = stages - 1

    def send(src, dst, ss, rs, target):
        return pltpu.make_async_remote_copy(src_ref=src, dst_ref=dst, send_sem=ss, recv_sem=rs, device_id=target, device_id_type=MESH_ID)

    barrier = pltpu.get_barrier_semaphore()
    for peer in (core_peer, x_peer, y_peer):
        pl.semaphore_signal(barrier, inc=1, device_id=(s, peer), device_id_type=MESH_ID)
    for off in range(1, stages):
        pl.semaphore_signal(barrier, inc=1, device_id=(lax.rem(s + off, stages), d), device_id_type=MESH_ID)

    def in_copy(n):
        unit, yx = n // 4, lax.rem(n, 4)
        slot = lax.rem(n, 2)
        return pltpu.make_async_copy(acc_in.at[layers - 1 - unit, pl.ds(yx * 128, 128), :], st_in.at[slot], sem_st_in.at[slot])

    def out_copy(n):
        unit, yx = n // 4, lax.rem(n, 4)
        slot = lax.rem(n, 2)
        return pltpu.make_async_copy(acc_out.at[layers - 1 - unit, pl.ds(yx * 512, 512), :], st_out.at[slot], sem_st_out.at[slot])

    part_rows = HALF_VOCAB * 4
    chunk_rows = VOCAB_CHUNK * 4
    tail_rows = vocab * 4 - (part_rows * 2 * stages - chunk_rows)

    def emb_copy(n, act):
        k, half = n // 2, n % 2
        slot = n % 2
        start = pl.multiple_of(s * (2 * part_rows) + half * part_rows + k * chunk_rows, 8)

        def full():
            act(pltpu.make_async_copy(acc_emb.at[pl.ds(start, chunk_rows), :], st_e.at[slot], sem_st_e.at[slot]))

        if k == CHUNKS - 1 and half == 1:
            @pl.when(s == last)
            def _():
                act(pltpu.make_async_copy(acc_emb.at[pl.ds(vocab * 4 - tail_rows, tail_rows), :],
                                          st_e.at[slot, pl.ds(0, tail_rows), :], sem_st_e.at[slot]))

            @pl.when(s != last)
            def _():
                full()
        else:
            full()

    w_copies = []
    for layer in range(layers):
        for j, (w, u) in enumerate(((w_in, u_in), (w_out, u_out))):
            w_copies.append(pltpu.make_async_copy(w.at[layer], u.at[layer], sem_w.at[2 * layer + j]))
            w_copies[-1].start()
    for n in range(2):
        in_copy(jnp.int32(n)).start()
        out_copy(jnp.int32(n)).start()
        emb_copy(n, lambda cp: cp.start())

    rows = cot_ref.shape[0]

    def dx_send(k, z):
        return send(dxb.at[k], dxb.at[k], dxs.at[k, z], dxr.at[k], (z, d))

    def cot_send(k, target):
        return send(cot_buf.at[k], cot_rcv.at[k], sem_cs.at[k], sem_cr.at[k], (target, d))

    def weight_produce(unit):
        layer = unit // 2
        if unit % 2 == 0:
            def body(yx, carry):
                n = 4 * (layers - 1 - layer) + yx
                slot = lax.rem(n, 2)
                in_copy(n).wait()
                lhs = x_ref[layer, :, pl.ds(pl.multiple_of(yx * 128, 128), 128)]
                for col in range(4):
                    cs = slice(col * 512, (col + 1) * 512)
                    new = lax.dot_general(lhs, dh_ref[layer, :, cs], (((0,), (0,)), ((), ())), preferred_element_type=F32)
                    tot = (st_in[slot, :, cs] + new).astype(BF)
                    u_in[layer, yx // 2, lax.rem(yx, 2), 0, :, cs] = tot[:64]
                    u_in[layer, yx // 2, lax.rem(yx, 2), 1, :, cs] = tot[64:]

                @pl.when(n + 2 < 12)
                def _():
                    in_copy(n + 2).start()
                return carry
        else:
            def body(yx, carry):
                n = 4 * (layers - 1 - layer) + yx
                slot = lax.rem(n, 2)
                out_copy(n).wait()
                for part in range(4):
                    rows = pl.ds(part * 128, 128)
                    lhs = h_ref[layer, :, pl.ds(pl.multiple_of(yx * 512 + part * 128, 128), 128)]
                    new = lax.dot_general(lhs, g_ref[layer], (((0,), (0,)), ((), ())), preferred_element_type=F32)
                    tot = (st_out[slot, rows, :] + new).astype(BF)
                    u_out[layer, yx // 2, lax.rem(yx, 2), part // 2, pl.ds((part % 2) * 128, 128), :] = tot

                @pl.when(n + 2 < 12)
                def _():
                    out_copy(n + 2).start()
                return carry
        lax.fori_loop(0, 4, body, 0)

    def emb_produce(k):
        for half in range(2):
            n = 2 * k + half
            emb_copy(n, lambda cp: cp.wait())

            def body(q, carry):
                u_e[k, q // 2, lax.rem(q, 2), half] = st_e[n % 2, pl.ds(q, VOCAB_CHUNK, stride=4), :].astype(BF)
                return carry
            lax.fori_loop(0, 4, body, 0)
            if n + 2 < 2 * CHUNKS:
                emb_copy(n + 2, lambda cp: cp.start())

    def touched_produce():
        @pl.when(s > 0)
        def _():
            for step in range(stages):
                dx_send(step, 0).wait_recv()
        for r in range(8):
            hot = (ids_ref[...] == slot_ref[r, pl.ds(last - s, 1), :]).astype(F32).astype(BF)
            for q in range(4):
                new = lax.dot_general(hot, dxb[:, q].reshape(128, 128), (((0,), (0,)), ((), ())), preferred_element_type=F32)
                old = touched_ref[pl.ds(r * 128 + q, 32, stride=4), :]
                u_t[q // 2, q % 2, r // 4, (r % 4) * 32:(r % 4 + 1) * 32, :] = (old + new).astype(BF)

    def unit_bufs(kind, i):
        if kind == 'e':
            return u_e.at[i], r0_e.at[i], r1_e.at[i], r2_e.at[i], VOCAB_CHUNK
        if kind == 't':
            return u_t, r0_t, r1_t, r2_t, 128
        if i % 2 == 0:
            return u_in.at[i // 2], r0_in.at[i // 2], r1_in.at[i // 2], r2_in.at[i // 2], 64
        return u_out.at[i // 2], r0_out.at[i // 2], r1_out.at[i // 2], r2_out.at[i // 2], 256

    def core_send(pos):
        u, r0, r1, r2, rows = unit_bufs(*UNIT_ORDER[pos])
        return send(u.at[:, :, 1 - c], r0, s0s.at[pos], s0r.at[pos], (s, core_peer))

    def first_send(pos):
        u, r0, r1, r2, rows = unit_bufs(*UNIT_ORDER[pos])
        if pos % 2 == 0:
            return send(u.at[:, 1 - x, c], r1, s1s.at[pos], s1r.at[pos], (s, x_peer))
        return send(u.at[1 - y, :, c], r1, s1s.at[pos], s1r.at[pos], (s, y_peer))

    def second_send(pos):
        u, r0, r1, r2, rows = unit_bufs(*UNIT_ORDER[pos])
        if pos % 2 == 0:
            return send(u.at[1 - y, x, c], r2, s2s.at[pos], s2r.at[pos], (s, y_peer))
        return send(u.at[y, 1 - x, c], r2, s2s.at[pos], s2r.at[pos], (s, x_peer))

    def stage_produce(pos):
        kind, i = UNIT_ORDER[pos]
        if kind == 'w':
            weight_produce(i)
        elif kind == 't':
            touched_produce()
        else:
            emb_produce(i)
        core_send(pos).start()

    def stage_add(pos):
        u, r0, r1, r2, rows = unit_bufs(*UNIT_ORDER[pos])
        core_send(pos).wait_recv()
        far = [(j, 1 - x) for j in range(2)] if pos % 2 == 0 else [(1 - y, j) for j in range(2)]
        near = [(j, x) for j in range(2)] if pos % 2 == 0 else [(y, j) for j in range(2)]
        for a, b in far:
            u[a, b, c] = u[a, b, c] + r0[a, b]
        first_send(pos).start()
        for a, b in near:
            u[a, b, c] = u[a, b, c] + r0[a, b]

    def stage_second(pos):
        u, r0, r1, r2, rows = unit_bufs(*UNIT_ORDER[pos])
        first_send(pos).wait_recv()
        far, i = ((1 - y, x), 1 - y) if pos % 2 == 0 else ((y, 1 - x), 1 - x)
        u[far[0], far[1], c] = u[far[0], far[1], c] + r1[i]
        second_send(pos).start()
        u[y, x, c] = u[y, x, c] + r1[1 - i]

    def piece(p, k):
        return agt.at[p] if k == TOUCH_GROUP else ag.at[p, pl.ds(*GROUPS[k])]

    def own_sends(k, act):
        for j, off in enumerate((1, -1) if k != TOUCH_GROUP else (1, -1, 2, -2, 3, -3)):
            @pl.when((s + off >= 0) & (s + off <= last))
            def _():
                blk = piece(2 * s + c, k)
                act(send(blk, blk, own_s.at[j, k], col_r.at[s, k], (jnp.clip(s + off, 0, last), d)))

    def far_send(k, hop, sign, act):
        z = s - sign * hop

        @pl.when((z >= 0) & (z <= last) & (s + sign >= 0) & (s + sign <= last))
        def _():
            zc = jnp.clip(z, 0, last)
            blk = piece(2 * zc + c, k)
            act(send(blk, blk, fwd_s.at[zc, k], col_r.at[zc, k], (jnp.clip(s + sign, 0, last), d)))

    def col_wait(z, k):
        blk = piece(2 * z + c, k)
        send(blk, blk, fwd_s.at[0, 0], col_r.at[z, k], (s, d)).wait_recv()

    def part_send(z, k):
        blk = piece(2 * z + c, k)
        return send(blk, blk, pt_s.at[z, k], pt_r.at[z, k], (s, core_peer))

    def emb_write(p, k):
        dst = patch_ref.at[p] if k == TOUCH_GROUP else emb_ref.at[p, pl.ds(*GROUPS[k])]
        return pltpu.make_async_copy(piece(p, k), dst, sem_t.at[p, k])

    def emit(p, k):
        emb_write(p, k).start()

    def have_piece(z, k):
        part_send(z, k).start()
        emit(2 * z + c, k)

    def stage_last(pos):
        kind, i = UNIT_ORDER[pos]
        u, r0, r1, r2, rows = unit_bufs(kind, i)
        second_send(pos).wait_recv()
        if kind == 'e':
            ag[2 * s + c, i] = u[y, x, c] + r2[...]
            for k, (first, count) in enumerate(GROUPS):
                if i == first + count - 1:
                    own_sends(k, lambda cp: cp.start())
                    have_piece(s, k)
        elif kind == 't':
            agt[2 * s + c] = u[y, x, c] + r2[...]
            own_sends(TOUCH_GROUP, lambda cp: cp.start())
            have_piece(s, TOUCH_GROUP)
        else:
            tot = (u[y, x, c].astype(F32) + r2[...].astype(F32))
            if i % 2 == 0:
                gin_ref[i // 2] = tot
            else:
                gout_ref[i // 2] = tot

    def part_event(z, k):
        part_send(z, k).wait_recv()
        emit(2 * z + 1 - c, k)

    def hop_event(k, hop):
        for sign in (-1, 1):
            z = s - sign * hop

            @pl.when((z >= 0) & (z <= last))
            def _():
                col_wait(jnp.clip(z, 0, last), k)
            if k != TOUCH_GROUP:
                far_send(k, hop, sign, lambda cp: cp.start())

            @pl.when((z >= 0) & (z <= last))
            def _():
                have_piece(jnp.clip(z, 0, last), k)

    events = [(k, hop) for hop in (1, 2, 3) for k in range(TOUCH_GROUP)]

    def run(slot):
        for op in slot:
            if op == 'h':
                hop_event(*events.pop(0))
            else:
                {'p': stage_produce, 'a': stage_add, 's': stage_second, 'l': stage_last}[op[0]](int(op[1:]))

    for k in range(stages):
        x_ref[0, k * rows:(k + 1) * rows, :] = stored_ref[jnp.maximum(last - s - k, 0)]
    pl.semaphore_wait(barrier, 3 + stages - 1)
    slots = list(CHAIN_SLOTS)
    run(slots.pop(0))
    for layer in range(layers):
        w_copies[2 * layer].wait()
        x_cur = x_ref[layer]
        for i in range(4):
            cs = slice(i * 512, (i + 1) * 512)
            pre = jnp.dot(x_cur, u_in[layer, :, :, :, :, cs].reshape(512, 512), preferred_element_type=F32).astype(BF)
            act, der = gelu_and_slope(pre.astype(F32))
            h_ref[layer, :, cs] = act.astype(BF)
            slope[layer, :, cs] = der
        run(slots.pop(0))
        w_copies[2 * layer + 1].wait()
        if layer < layers - 1:
            out = jnp.dot(h_ref[layer], u_out[layer].reshape(2048, 512), preferred_element_type=F32)
            x_ref[layer + 1] = (x_cur.astype(F32) + out).astype(BF)
        run(slots.pop(0))

    for k in range(stages):
        rs = slice(k * rows, (k + 1) * rows)
        active = s + k <= last
        for layer in range(layers - 1, -1, -1):
            @pl.when(active)
            def _():
                if layer < layers - 1:
                    cot = g_ref[layer, rs, :]
                else:
                    if k > 0:
                        cot_send(k - 1, s).wait_recv()
                        cot = cot_rcv[k - 1]
                    else:
                        cot = cot_ref[...]
                    g_ref[layer, rs, :] = cot
                back = cot.astype(F32)
                for i in range(4):
                    cs = slice(i * 512, (i + 1) * 512)
                    dh = lax.dot_general(cot, u_out[layer, i // 2, i % 2].reshape(512, 512), (((1,), (1,)), ((), ())), preferred_element_type=F32).astype(BF)
                    dh = (dh.astype(F32) * slope[layer, rs, cs]).astype(BF)
                    dh_ref[layer, rs, cs] = dh
                    back = back + lax.dot_general(dh, u_in[layer, :, :, :, :, cs].reshape(512, 512), (((1,), (1,)), ((), ())), preferred_element_type=F32)
                cot = back.astype(BF)
                if layer > 0:
                    g_ref[layer - 1, rs, :] = cot
                else:
                    cot_buf[k] = cot

                    @pl.when(s > 0)
                    def _():
                        cot_send(k, jnp.maximum(s - 1, 0)).start()

                    @pl.when(s == 0)
                    def _():
                        for q in range(4):
                            dxb[k, q] = cot[:, q * 128:(q + 1) * 128]
                        for z in range(1, stages):
                            dx_send(k, z).start()

            @pl.when(jnp.logical_not(active))
            def _():
                g_ref[layer, rs, :] = jnp.zeros((rows, 512), BF)
                dh_ref[layer, rs, :] = jnp.zeros((rows, 2048), BF)
            run(slots.pop(0))

    total = len(UNIT_ORDER)
    for slot in TAIL_SLOTS:
        run(slot)
    for hop in (1, 2, 3):
        hop_event(TOUCH_GROUP, hop)

    for k in range(TOUCH_GROUP + 1):
        for z in range(stages):
            part_event(z, k)

    for pos in range(total):
        core_send(pos).wait_send()
        first_send(pos).wait_send()
        second_send(pos).wait_send()

    for k in range(stages):
        @pl.when(s == 0)
        def _():
            for z in range(1, stages):
                dx_send(k, z).wait_send()

        @pl.when((s > 0) & (s + k <= last))
        def _():
            cot_send(k, jnp.maximum(s - 1, 0)).wait_send()

    def drain(z, k):
        part_send(z, k).wait_send()
        for core in range(2):
            emb_write(2 * z + core, k).wait()

    for k in range(TOUCH_GROUP + 1):
        for z in range(stages):
            drain(z, k)
    for k in range(TOUCH_GROUP + 1):
        own_sends(k, lambda cp: cp.wait_send())
        if k != TOUCH_GROUP:
            for hop in (1, 2):
                for sign in (-1, 1):
                    far_send(k, hop, sign, lambda cp: cp.wait_send())


def share_kernel(replicas, own_ref, all_ref, buf, send_sem, recv_sem):
    s = lax.axis_index('pp')
    d = lax.axis_index('dp')
    barrier = pltpu.get_barrier_semaphore()
    for off in range(1, replicas):
        pl.semaphore_signal(barrier, inc=1, device_id=(s, lax.rem(d + off, replicas)), device_id_type=MESH_ID)
    pl.semaphore_wait(barrier, replicas - 1)

    def copy(off):
        return pltpu.make_async_remote_copy(src_ref=own_ref, dst_ref=buf.at[d], send_sem=send_sem.at[off], recv_sem=recv_sem.at[d],
                                            device_id=(s, lax.rem(d + off, replicas)), device_id_type=MESH_ID)
    for off in range(1, replicas):
        copy(off).start()
    buf[d] = own_ref[...]
    for off in range(1, replicas):
        src = lax.rem(d + off, replicas)
        pltpu.make_async_remote_copy(src_ref=own_ref, dst_ref=buf.at[src], send_sem=send_sem.at[off], recv_sem=recv_sem.at[src],
                                     device_id=(s, src), device_id_type=MESH_ID).wait_recv()
    for off in range(1, replicas):
        copy(off).wait_send()
    all_ref[...] = buf[...]


def gather_kernel(ids_ref, emb_ref, out_ref, sem):
    replicas, _, tokens = ids_ref.shape
    z = ids_ref.shape[1] - 1 - lax.axis_index('pp')

    def body(i, carry):
        r, t = i // (tokens // 8), lax.rem(i, tokens // 8) * 8
        for j in range(8):
            pltpu.make_async_copy(emb_ref.at[ids_ref[r, z, t + j]], out_ref.at[i * 8 + j], sem).start()
        return carry
    lax.fori_loop(0, replicas * tokens // 8, body, 0)
    pltpu.make_async_copy(emb_ref.at[pl.ds(0, replicas * tokens)], out_ref, sem).wait()


def finish_kernel(scale, ids_ref, base_ref, patch_ref, gin_ref, gout_ref, emb_out, gin_out, gout_out, rows_f, patch_f, stage, gin_buf, gout_buf, sem, sem_g):
    step = pl.program_id(0)
    core = lax.rem(lax.axis_index('dp'), 2)
    chunks = base_ref.shape[0]
    moves = ((gin_ref, gin_out, gin_buf, 0), (gout_ref, gout_out, gout_buf, 1))

    @pl.when(step == 0)
    def _():
        def copy(i):
            return pltpu.make_async_copy(base_ref.at[i], stage.at[pl.ds(pl.multiple_of(i * VOCAB_CHUNK, VOCAB_CHUNK), VOCAB_CHUNK), :], sem.at[i])
        for i in range(chunks):
            copy(i).start()
        for src, dst, buf, j in moves:
            pltpu.make_async_copy(src, buf, sem_g.at[j]).start()
        patch_f[...] = patch_ref[...].astype(F32)

        def widen(i, carry):
            copy(i).wait()
            chunk = pl.ds(pl.multiple_of(i * VOCAB_CHUNK, VOCAB_CHUNK), VOCAB_CHUNK)
            rows_f[chunk, :] = stage[chunk, :].astype(F32)
            return carry
        lax.fori_loop(0, chunks, widen, 0)

        replicas, stages, tokens = ids_ref.shape

        for z in range(stages):
            def put(r, carry):
                row = pl.multiple_of((z * replicas + r) * tokens, tokens)
                rows = patch_f[pl.ds(row, tokens), :]
                for t in range(tokens):
                    rows_f[pl.ds(ids_ref[r, stages - 1 - z, t], 1), :] = rows[t:t + 1, :]
                return carry
            lax.fori_loop(0, replicas, put, 0)

    @pl.when(step == 1)
    def _():
        for src, dst, buf, j in moves:
            pltpu.make_async_copy(src, buf, sem_g.at[j]).wait()
            buf[...] = buf[...] * scale
            pltpu.make_async_copy(buf, dst, sem_g.at[2 + j]).start()

    @pl.when(step == pl.num_programs(0) - 1)
    def _():
        for src, dst, buf, j in moves:
            pltpu.make_async_copy(buf, dst, sem_g.at[2 + j]).wait()

    pick = lax.broadcasted_iota(jnp.int32, (64, 128), 1) == lax.broadcasted_iota(jnp.int32, (64, 128), 0) + 64 * core
    sel = jnp.where(pick, scale, 0.0).astype(BF)
    for i in range(FINISH_BLOCK // VOCAB_CHUNK):
        start = pl.multiple_of(step * FINISH_BLOCK + i * VOCAB_CHUNK, VOCAB_CHUNK)
        block = rows_f[pl.ds(start, VOCAB_CHUNK), :].astype(BF)
        emb_out[:, i * VOCAB_CHUNK:(i + 1) * VOCAB_CHUNK] = lax.dot_general(sel, block, (((1,), (1,)), ((), ())), preferred_element_type=F32)


def solution(mesh):
    stages = mesh.shape['pp']
    replicas = mesh.shape['dp']

    def device_body(tok_ids, d_out, stored_x, w_in, w_out, acc_in, acc_out, acc_emb):
        layers, hid, ff = w_in.shape
        vocab = acc_emb.shape[1]
        tokens = d_out.shape[1]
        rows = tokens * stages
        ids = tok_ids[::-1].reshape(rows, 1)
        vm = pl.BlockSpec(memory_space=pltpu.VMEM)
        hbm = pl.BlockSpec(memory_space=pltpu.HBM)
        smem = pl.BlockSpec(memory_space=pltpu.SMEM)
        dma = pltpu.SemaphoreType.DMA
        slot_ids = pl.pallas_call(
            functools.partial(share_kernel, replicas),
            out_shape=jax.ShapeDtypeStruct((replicas, stages, tokens), jnp.int32),
            in_specs=[vm], out_specs=vm,
            scratch_shapes=[pltpu.VMEM((replicas, stages, tokens), jnp.int32), dma((replicas,)), dma((replicas,))],
            compiler_params=pltpu.CompilerParams(collective_id=1, has_side_effects=True),
            name='share_ids',
        )(tok_ids)
        touched = pl.pallas_call(
            gather_kernel,
            out_shape=jax.ShapeDtypeStruct((replicas * tokens, 4, 128), F32),
            in_specs=[smem, hbm], out_specs=vm, scratch_shapes=[pltpu.SemaphoreType.DMA],
            name='gather_rows',
        )(slot_ids, acc_emb.reshape(vocab, 4, 128))
        v = pltpu.VMEM
        dma = pltpu.SemaphoreType.DMA
        units = len(UNIT_ORDER)
        gin, gout, emb, patch = pl.pallas_call(
            functools.partial(comm_kernel, stages, layers, vocab),
            out_shape=(jax.ShapeDtypeStruct((layers, hid // 8, ff), F32), jax.ShapeDtypeStruct((layers, ff // 8, hid), F32),
                       jax.ShapeDtypeStruct((2 * stages, CHUNKS, VOCAB_CHUNK, 128), BF), jax.ShapeDtypeStruct((2 * stages, 128, 128), BF)),
            in_specs=[vm] * 5 + [hbm] * 5,
            out_specs=(vm, vm, hbm, hbm),
            scratch_shapes=[
                v((layers, rows, hid), BF), v((layers, rows, ff), BF), v((layers, rows, hid), BF), v((layers, rows, ff), BF), v((layers, rows, ff), F32),
                v((stages, tokens, hid), BF), v((stages, tokens, hid), BF), dma((2 * layers,)), dma((stages,)), dma((stages,)),
                v((layers, 2, 2, 2, 64, ff), BF), v((layers, 2, 2, 64, ff), BF), v((layers, 2, 64, ff), BF), v((layers, 64, ff), BF),
                v((layers, 2, 2, 2, 256, hid), BF), v((layers, 2, 2, 256, hid), BF), v((layers, 2, 256, hid), BF), v((layers, 256, hid), BF),
                v((CHUNKS, 2, 2, 2, VOCAB_CHUNK, 128), BF), v((CHUNKS, 2, 2, VOCAB_CHUNK, 128), BF), v((CHUNKS, 2, VOCAB_CHUNK, 128), BF), v((CHUNKS, VOCAB_CHUNK, 128), BF),
                v((2, 2, 2, 128, 128), BF), v((2, 2, 128, 128), BF), v((2, 128, 128), BF), v((128, 128), BF),
                v((2 * stages, CHUNKS, VOCAB_CHUNK, 128), BF), v((2 * stages, 128, 128), BF), v((stages, 4, tokens, 128), BF),
                v((2, 128, ff), F32), v((2, 512, hid), F32), v((2, VOCAB_CHUNK * 4, 128), F32),
                dma((2,)), dma((2,)), dma((2,)), dma((2 * stages, CHUNKS + 1)),
                dma((units,)), dma((units,)), dma((units,)), dma((units,)), dma((units,)), dma((units,)),
                dma((stages, stages)), dma((stages,)), dma((6, CHUNKS + 1)), dma((stages, CHUNKS)), dma((stages, CHUNKS + 1)), dma((stages, CHUNKS + 1)), dma((stages, CHUNKS + 1)),
            ],
            compiler_params=pltpu.CompilerParams(collective_id=0, has_side_effects=True, vmem_limit_bytes=67043328),
            name='reduce_exchange',
        )(ids, slot_ids, touched.reshape(-1, 128), d_out[0], stored_x[0], w_in.reshape(layers, 2, 2, 2, 64, ff), w_out.reshape(layers, 2, 2, 2, 256, hid), acc_in.reshape(layers, hid, ff), acc_out.reshape(layers, ff, hid), acc_emb.reshape(vocab * 4, 128))
        grad_emb, grad_in, grad_out = pl.pallas_call(
            functools.partial(finish_kernel, 1.0 / replicas),
            out_shape=(jax.ShapeDtypeStruct((64, vocab), F32), jax.ShapeDtypeStruct(gin.shape, F32), jax.ShapeDtypeStruct(gout.shape, F32)),
            grid=(2 * stages * HALF_VOCAB // FINISH_BLOCK,),
            in_specs=[smem, hbm, vm, hbm, hbm],
            out_specs=(pl.BlockSpec((64, FINISH_BLOCK), lambda i: (0, i)), hbm, hbm),
            scratch_shapes=[v((2 * stages * CHUNKS * VOCAB_CHUNK, 128), F32), v((stages * replicas * tokens, 128), F32),
                            v((2 * stages * CHUNKS * VOCAB_CHUNK, 128), BF), v(gin.shape, F32), v(gout.shape, F32), dma((2 * stages * CHUNKS,)), dma((4,))],
            compiler_params=pltpu.CompilerParams(vmem_limit_bytes=58 * 2 ** 20, dimension_semantics=('arbitrary',)),
            name='finish',
        )(slot_ids, emb.reshape(2 * stages * CHUNKS, VOCAB_CHUNK, 128), patch.reshape(-1, 128), gin, gout)
        return grad_in, grad_out, grad_emb.T

    return jax.shard_map(device_body, mesh=mesh, in_specs=(P(None, 'dp'), P('pp', 'dp', None), P('pp', None, 'dp', None), P('pp', None, None), P('pp', None, None), P('pp', 'dp', None, None), P('pp', 'dp', None, None), P('dp', None, None)), out_specs=(P('pp', 'dp', None), P('pp', 'dp', None), P(None, 'dp')), check_vma=False)
```

```python
import functools

import jax
import jax.numpy as jnp
from jax import lax
from jax.experimental import pallas as pl
from jax.experimental.pallas import tpu as pltpu
from jax.sharding import PartitionSpec as P

MESH_ID = pl.DeviceIdType.MESH
BF = jnp.bfloat16
F32 = jnp.float32

VOCAB_CHUNK = 768
CHUNKS = 5
HALF_VOCAB = VOCAB_CHUNK * CHUNKS
WEIGHT_UNITS = 6
FINISH_BLOCK = 7680
UNIT_ORDER = tuple(('e', i) for i in range(CHUNKS)) + (('w', 5), ('w', 4), ('t', 0), ('w', 3), ('w', 2), ('w', 1), ('w', 0))
GROUPS = ((0, 1), (1, 1), (2, 1), (3, 1), (4, 1))
TOUCH_GROUP = len(GROUPS)
CHAIN_SLOTS = (
    ('p0',),
    ('p1',),
    ('a0', 'p2'),
    ('a1', 'p3'),
    ('a2', 'p4'),
    (),
    (),
    (),
    (),
    ('s0', 'a3', 's1', 'a4'),
    (),
    (),
    ('l0', 's2'),
    ('l1',),
    (),
    ('s3', 'h'),
    ('s4', 'l2', 'p5', 'h', 'p6'),
    ('a5', 'l3'),
    ('a6', 'l4', 'h', 'p7', 'p8', 'a7'),
)
TAIL_SLOTS = (
    ('p9', 'p10', 'h', 'a8', 'p11', 'h', 'a9', 's5', 's7', 'h', 's6'),
    ('a11', 'a10', 'h', 'h', 's9', 's8', 'h'),
    ('l6', 'l5', 'l7', 'h'),
    ('s11', 's10', 'h', 'h', 'h'),
    ('l8', 'l9', 'h'),
    ('l10', 'h'),
    ('l11',),
)


def gelu_and_slope(pre):
    return jax.jvp(jax.nn.gelu, (pre,), (jnp.ones_like(pre),))


def comm_kernel(stages, layers, vocab, ids_ref, slot_ref, touched_ref, cot_ref, stored_ref, w_in, w_out, acc_in, acc_out, acc_emb,
                gin_ref, gout_ref, emb_ref, patch_ref, x_ref, h_ref, g_ref, dh_ref, slope, cot_buf, cot_rcv,
                sem_w, sem_cs, sem_cr,
                u_in, r0_in, r1_in, r2_in, u_out, r0_out, r1_out, r2_out, u_e, r0_e, r1_e, r2_e, u_t, r0_t, r1_t, r2_t,
                ag, agt, dxb, st_in, st_out, st_e,
                sem_st_in, sem_st_out, sem_st_e, sem_t, s0s, s0r, s1s, s1r, s2s, s2r,
                dxs, dxr, own_s, fwd_s, pt_s, col_r, pt_r):
    s = lax.axis_index('pp')
    d = lax.axis_index('dp')
    c = lax.rem(d, 2)
    x = lax.rem(d // 2, 2)
    y = d // 4
    core_peer = d + 1 - 2 * c
    x_peer = d + 2 - 4 * x
    y_peer = d + 4 - 8 * y
    last = stages - 1

    def send(src, dst, ss, rs, target):
        return pltpu.make_async_remote_copy(src_ref=src, dst_ref=dst, send_sem=ss, recv_sem=rs, device_id=target, device_id_type=MESH_ID)

    barrier = pltpu.get_barrier_semaphore()
    for peer in (core_peer, x_peer, y_peer):
        pl.semaphore_signal(barrier, inc=1, device_id=(s, peer), device_id_type=MESH_ID)
    for off in range(1, stages):
        pl.semaphore_signal(barrier, inc=1, device_id=(lax.rem(s + off, stages), d), device_id_type=MESH_ID)

    def in_copy(n):
        unit, yx = n // 4, lax.rem(n, 4)
        slot = lax.rem(n, 2)
        return pltpu.make_async_copy(acc_in.at[layers - 1 - unit, pl.ds(yx * 128, 128), :], st_in.at[slot], sem_st_in.at[slot])

    def out_copy(n):
        unit, yx = n // 4, lax.rem(n, 4)
        slot = lax.rem(n, 2)
        return pltpu.make_async_copy(acc_out.at[layers - 1 - unit, pl.ds(yx * 512, 512), :], st_out.at[slot], sem_st_out.at[slot])

    part_rows = HALF_VOCAB * 4
    chunk_rows = VOCAB_CHUNK * 4
    tail_rows = vocab * 4 - (part_rows * 2 * stages - chunk_rows)

    def emb_copy(n, act):
        k, half = n // 2, n % 2
        slot = n % 2
        start = pl.multiple_of(s * (2 * part_rows) + half * part_rows + k * chunk_rows, 8)

        def full():
            act(pltpu.make_async_copy(acc_emb.at[pl.ds(start, chunk_rows), :], st_e.at[slot], sem_st_e.at[slot]))

        if k == CHUNKS - 1 and half == 1:
            @pl.when(s == last)
            def _():
                act(pltpu.make_async_copy(acc_emb.at[pl.ds(vocab * 4 - tail_rows, tail_rows), :],
                                          st_e.at[slot, pl.ds(0, tail_rows), :], sem_st_e.at[slot]))

            @pl.when(s != last)
            def _():
                full()
        else:
            full()

    w_copies = []
    for layer in range(layers):
        for j, (w, u) in enumerate(((w_in, u_in), (w_out, u_out))):
            w_copies.append(pltpu.make_async_copy(w.at[layer], u.at[layer], sem_w.at[2 * layer + j]))
            w_copies[-1].start()
    for n in range(2):
        in_copy(jnp.int32(n)).start()
        out_copy(jnp.int32(n)).start()
        emb_copy(n, lambda cp: cp.start())

    rows = cot_ref.shape[0]

    def dx_send(k, z):
        return send(dxb.at[k], dxb.at[k], dxs.at[k, z], dxr.at[k], (z, d))

    def cot_send(k, target):
        return send(cot_buf.at[k], cot_rcv.at[k], sem_cs.at[k], sem_cr.at[k], (target, d))

    def weight_produce(unit):
        layer = unit // 2
        if unit % 2 == 0:
            def body(yx, carry):
                n = 4 * (layers - 1 - layer) + yx
                slot = lax.rem(n, 2)
                in_copy(n).wait()
                lhs = x_ref[layer, :, pl.ds(pl.multiple_of(yx * 128, 128), 128)]
                for col in range(4):
                    cs = slice(col * 512, (col + 1) * 512)
                    new = lax.dot_general(lhs, dh_ref[layer, :, cs], (((0,), (0,)), ((), ())), preferred_element_type=F32)
                    tot = (st_in[slot, :, cs] + new).astype(BF)
                    u_in[layer, yx // 2, lax.rem(yx, 2), 0, :, cs] = tot[:64]
                    u_in[layer, yx // 2, lax.rem(yx, 2), 1, :, cs] = tot[64:]

                @pl.when(n + 2 < 12)
                def _():
                    in_copy(n + 2).start()
                return carry
        else:
            def body(yx, carry):
                n = 4 * (layers - 1 - layer) + yx
                slot = lax.rem(n, 2)
                out_copy(n).wait()
                for part in range(4):
                    rows = pl.ds(part * 128, 128)
                    lhs = h_ref[layer, :, pl.ds(pl.multiple_of(yx * 512 + part * 128, 128), 128)]
                    new = lax.dot_general(lhs, g_ref[layer], (((0,), (0,)), ((), ())), preferred_element_type=F32)
                    tot = (st_out[slot, rows, :] + new).astype(BF)
                    u_out[layer, yx // 2, lax.rem(yx, 2), part // 2, pl.ds((part % 2) * 128, 128), :] = tot

                @pl.when(n + 2 < 12)
                def _():
                    out_copy(n + 2).start()
                return carry
        lax.fori_loop(0, 4, body, 0)

    def emb_produce(k):
        for half in range(2):
            n = 2 * k + half
            emb_copy(n, lambda cp: cp.wait())

            def body(q, carry):
                u_e[k, q // 2, lax.rem(q, 2), half] = st_e[n % 2, pl.ds(q, VOCAB_CHUNK, stride=4), :].astype(BF)
                return carry
            lax.fori_loop(0, 4, body, 0)
            if n + 2 < 2 * CHUNKS:
                emb_copy(n + 2, lambda cp: cp.start())

    def touched_produce():
        @pl.when(s > 0)
        def _():
            for step in range(stages):
                dx_send(step, 0).wait_recv()
        for r in range(8):
            hot = (ids_ref[...] == slot_ref[r, pl.ds(last - s, 1), :]).astype(F32).astype(BF)
            for q in range(4):
                new = lax.dot_general(hot, dxb[:, q].reshape(128, 128), (((0,), (0,)), ((), ())), preferred_element_type=F32)
                old = touched_ref[pl.ds(r * 128 + q, 32, stride=4), :]
                u_t[q // 2, q % 2, r // 4, (r % 4) * 32:(r % 4 + 1) * 32, :] = (old + new).astype(BF)

    def unit_bufs(kind, i):
        if kind == 'e':
            return u_e.at[i], r0_e.at[i], r1_e.at[i], r2_e.at[i], VOCAB_CHUNK
        if kind == 't':
            return u_t, r0_t, r1_t, r2_t, 128
        if i % 2 == 0:
            return u_in.at[i // 2], r0_in.at[i // 2], r1_in.at[i // 2], r2_in.at[i // 2], 64
        return u_out.at[i // 2], r0_out.at[i // 2], r1_out.at[i // 2], r2_out.at[i // 2], 256

    def core_send(pos):
        u, r0, r1, r2, rows = unit_bufs(*UNIT_ORDER[pos])
        return send(u.at[:, :, 1 - c], r0, s0s.at[pos], s0r.at[pos], (s, core_peer))

    def first_send(pos):
        u, r0, r1, r2, rows = unit_bufs(*UNIT_ORDER[pos])
        if pos % 2 == 0:
            return send(u.at[:, 1 - x, c], r1, s1s.at[pos], s1r.at[pos], (s, x_peer))
        return send(u.at[1 - y, :, c], r1, s1s.at[pos], s1r.at[pos], (s, y_peer))

    def second_send(pos):
        u, r0, r1, r2, rows = unit_bufs(*UNIT_ORDER[pos])
        if pos % 2 == 0:
            return send(u.at[1 - y, x, c], r2, s2s.at[pos], s2r.at[pos], (s, y_peer))
        return send(u.at[y, 1 - x, c], r2, s2s.at[pos], s2r.at[pos], (s, x_peer))

    def stage_produce(pos):
        kind, i = UNIT_ORDER[pos]
        if kind == 'w':
            weight_produce(i)
        elif kind == 't':
            touched_produce()
        else:
            emb_produce(i)
        core_send(pos).start()

    def stage_add(pos):
        u, r0, r1, r2, rows = unit_bufs(*UNIT_ORDER[pos])
        core_send(pos).wait_recv()
        far = [(j, 1 - x) for j in range(2)] if pos % 2 == 0 else [(1 - y, j) for j in range(2)]
        near = [(j, x) for j in range(2)] if pos % 2 == 0 else [(y, j) for j in range(2)]
        for a, b in far:
            u[a, b, c] = u[a, b, c] + r0[a, b]
        first_send(pos).start()
        for a, b in near:
            u[a, b, c] = u[a, b, c] + r0[a, b]

    def stage_second(pos):
        u, r0, r1, r2, rows = unit_bufs(*UNIT_ORDER[pos])
        first_send(pos).wait_recv()
        far, i = ((1 - y, x), 1 - y) if pos % 2 == 0 else ((y, 1 - x), 1 - x)
        u[far[0], far[1], c] = u[far[0], far[1], c] + r1[i]
        second_send(pos).start()
        u[y, x, c] = u[y, x, c] + r1[1 - i]

    def piece(p, k):
        return agt.at[p] if k == TOUCH_GROUP else ag.at[p, pl.ds(*GROUPS[k])]

    def own_sends(k, act):
        for j, off in enumerate((1, -1) if k != TOUCH_GROUP else (1, -1, 2, -2, 3, -3)):
            @pl.when((s + off >= 0) & (s + off <= last))
            def _():
                blk = piece(2 * s + c, k)
                act(send(blk, blk, own_s.at[j, k], col_r.at[s, k], (jnp.clip(s + off, 0, last), d)))

    def far_send(k, hop, sign, act):
        z = s - sign * hop

        @pl.when((z >= 0) & (z <= last) & (s + sign >= 0) & (s + sign <= last))
        def _():
            zc = jnp.clip(z, 0, last)
            blk = piece(2 * zc + c, k)
            act(send(blk, blk, fwd_s.at[zc, k], col_r.at[zc, k], (jnp.clip(s + sign, 0, last), d)))

    def col_wait(z, k):
        blk = piece(2 * z + c, k)
        send(blk, blk, fwd_s.at[0, 0], col_r.at[z, k], (s, d)).wait_recv()

    def part_send(z, k):
        blk = piece(2 * z + c, k)
        return send(blk, blk, pt_s.at[z, k], pt_r.at[z, k], (s, core_peer))

    def emb_write(p, k):
        dst = patch_ref.at[p] if k == TOUCH_GROUP else emb_ref.at[p, pl.ds(*GROUPS[k])]
        return pltpu.make_async_copy(piece(p, k), dst, sem_t.at[p, k])

    def emit(p, k):
        emb_write(p, k).start()

    def have_piece(z, k):
        part_send(z, k).start()
        emit(2 * z + c, k)

    def stage_last(pos):
        kind, i = UNIT_ORDER[pos]
        u, r0, r1, r2, rows = unit_bufs(kind, i)
        second_send(pos).wait_recv()
        if kind == 'e':
            ag[2 * s + c, i] = u[y, x, c] + r2[...]
            for k, (first, count) in enumerate(GROUPS):
                if i == first + count - 1:
                    own_sends(k, lambda cp: cp.start())
                    have_piece(s, k)
        elif kind == 't':
            agt[2 * s + c] = u[y, x, c] + r2[...]
            own_sends(TOUCH_GROUP, lambda cp: cp.start())
            have_piece(s, TOUCH_GROUP)
        else:
            tot = (u[y, x, c].astype(F32) + r2[...].astype(F32))
            if i % 2 == 0:
                gin_ref[i // 2] = tot
            else:
                gout_ref[i // 2] = tot

    def part_event(z, k):
        part_send(z, k).wait_recv()
        emit(2 * z + 1 - c, k)

    def hop_event(k, hop):
        for sign in (-1, 1):
            z = s - sign * hop

            @pl.when((z >= 0) & (z <= last))
            def _():
                col_wait(jnp.clip(z, 0, last), k)
            if k != TOUCH_GROUP:
                far_send(k, hop, sign, lambda cp: cp.start())

            @pl.when((z >= 0) & (z <= last))
            def _():
                have_piece(jnp.clip(z, 0, last), k)

    events = [(k, hop) for hop in (1, 2, 3) for k in range(TOUCH_GROUP)]

    def run(slot):
        for op in slot:
            if op == 'h':
                hop_event(*events.pop(0))
            else:
                {'p': stage_produce, 'a': stage_add, 's': stage_second, 'l': stage_last}[op[0]](int(op[1:]))

    for k in range(stages):
        x_ref[0, k * rows:(k + 1) * rows, :] = stored_ref[jnp.maximum(last - s - k, 0)]
    pl.semaphore_wait(barrier, 3 + stages - 1)
    slots = list(CHAIN_SLOTS)
    run(slots.pop(0))
    for layer in range(layers):
        w_copies[2 * layer].wait()
        x_cur = x_ref[layer]
        for i in range(4):
            cs = slice(i * 512, (i + 1) * 512)
            pre = jnp.dot(x_cur, u_in[layer, :, :, :, :, cs].reshape(512, 512), preferred_element_type=F32).astype(BF)
            act, der = gelu_and_slope(pre.astype(F32))
            h_ref[layer, :, cs] = act.astype(BF)
            slope[layer, :, cs] = der
        run(slots.pop(0))
        w_copies[2 * layer + 1].wait()
        if layer < layers - 1:
            out = jnp.dot(h_ref[layer], u_out[layer].reshape(2048, 512), preferred_element_type=F32)
            x_ref[layer + 1] = (x_cur.astype(F32) + out).astype(BF)
        run(slots.pop(0))

    for k in range(stages):
        rs = slice(k * rows, (k + 1) * rows)
        active = s + k <= last
        for layer in range(layers - 1, -1, -1):
            @pl.when(active)
            def _():
                if layer < layers - 1:
                    cot = g_ref[layer, rs, :]
                else:
                    if k > 0:
                        cot_send(k - 1, s).wait_recv()
                        cot = cot_rcv[k - 1]
                    else:
                        cot = cot_ref[...]
                    g_ref[layer, rs, :] = cot
                back = cot.astype(F32)
                for i in range(4):
                    cs = slice(i * 512, (i + 1) * 512)
                    dh = lax.dot_general(cot, u_out[layer, i // 2, i % 2].reshape(512, 512), (((1,), (1,)), ((), ())), preferred_element_type=F32).astype(BF)
                    dh = (dh.astype(F32) * slope[layer, rs, cs]).astype(BF)
                    dh_ref[layer, rs, cs] = dh
                    back = back + lax.dot_general(dh, u_in[layer, :, :, :, :, cs].reshape(512, 512), (((1,), (1,)), ((), ())), preferred_element_type=F32)
                cot = back.astype(BF)
                if layer > 0:
                    g_ref[layer - 1, rs, :] = cot
                else:
                    cot_buf[k] = cot

                    @pl.when(s > 0)
                    def _():
                        cot_send(k, jnp.maximum(s - 1, 0)).start()

                    @pl.when(s == 0)
                    def _():
                        for q in range(4):
                            dxb[k, q] = cot[:, q * 128:(q + 1) * 128]
                        for z in range(1, stages):
                            dx_send(k, z).start()

            @pl.when(jnp.logical_not(active))
            def _():
                g_ref[layer, rs, :] = jnp.zeros((rows, 512), BF)
                dh_ref[layer, rs, :] = jnp.zeros((rows, 2048), BF)
            run(slots.pop(0))

    total = len(UNIT_ORDER)
    for slot in TAIL_SLOTS:
        run(slot)
    for hop in (1, 2, 3):
        hop_event(TOUCH_GROUP, hop)

    for k in range(TOUCH_GROUP + 1):
        for z in range(stages):
            part_event(z, k)

    for pos in range(total):
        core_send(pos).wait_send()
        first_send(pos).wait_send()
        second_send(pos).wait_send()

    for k in range(stages):
        @pl.when(s == 0)
        def _():
            for z in range(1, stages):
                dx_send(k, z).wait_send()

        @pl.when((s > 0) & (s + k <= last))
        def _():
            cot_send(k, jnp.maximum(s - 1, 0)).wait_send()

    def drain(z, k):
        part_send(z, k).wait_send()
        for core in range(2):
            emb_write(2 * z + core, k).wait()

    for k in range(TOUCH_GROUP + 1):
        for z in range(stages):
            drain(z, k)
    for k in range(TOUCH_GROUP + 1):
        own_sends(k, lambda cp: cp.wait_send())
        if k != TOUCH_GROUP:
            for hop in (1, 2):
                for sign in (-1, 1):
                    far_send(k, hop, sign, lambda cp: cp.wait_send())


def share_kernel(replicas, own_ref, all_ref, buf, send_sem, recv_sem):
    s = lax.axis_index('pp')
    d = lax.axis_index('dp')
    barrier = pltpu.get_barrier_semaphore()
    for off in range(1, replicas):
        pl.semaphore_signal(barrier, inc=1, device_id=(s, lax.rem(d + off, replicas)), device_id_type=MESH_ID)
    pl.semaphore_wait(barrier, replicas - 1)

    def copy(off):
        return pltpu.make_async_remote_copy(src_ref=own_ref, dst_ref=buf.at[d], send_sem=send_sem.at[off], recv_sem=recv_sem.at[d],
                                            device_id=(s, lax.rem(d + off, replicas)), device_id_type=MESH_ID)
    for off in range(1, replicas):
        copy(off).start()
    buf[d] = own_ref[...]
    for off in range(1, replicas):
        src = lax.rem(d + off, replicas)
        pltpu.make_async_remote_copy(src_ref=own_ref, dst_ref=buf.at[src], send_sem=send_sem.at[off], recv_sem=recv_sem.at[src],
                                     device_id=(s, src), device_id_type=MESH_ID).wait_recv()
    for off in range(1, replicas):
        copy(off).wait_send()
    all_ref[...] = buf[...]


def gather_kernel(ids_ref, emb_ref, out_ref, sem):
    replicas, _, tokens = ids_ref.shape
    z = ids_ref.shape[1] - 1 - lax.axis_index('pp')

    def body(r, carry):
        for t in range(tokens):
            pltpu.make_async_copy(emb_ref.at[ids_ref[r, z, t]], out_ref.at[r * tokens + t], sem).start()
        return carry
    lax.fori_loop(0, replicas, body, 0)
    pltpu.make_async_copy(emb_ref.at[pl.ds(0, replicas * tokens)], out_ref, sem).wait()


def finish_kernel(scale, ids_ref, base_ref, patch_ref, gin_ref, gout_ref, emb_out, gin_out, gout_out, rows_f, patch_f, stage, gin_buf, gout_buf, sem, sem_g):
    step = pl.program_id(0)
    core = lax.rem(lax.axis_index('dp'), 2)
    chunks = base_ref.shape[0]
    moves = ((gin_ref, gin_out, gin_buf, 0), (gout_ref, gout_out, gout_buf, 1))

    @pl.when(step == 0)
    def _():
        def copy(i):
            return pltpu.make_async_copy(base_ref.at[i], stage.at[pl.ds(pl.multiple_of(i * VOCAB_CHUNK, VOCAB_CHUNK), VOCAB_CHUNK), :], sem.at[i])
        for i in range(chunks):
            copy(i).start()
        for src, dst, buf, j in moves:
            pltpu.make_async_copy(src, buf, sem_g.at[j]).start()
        patch_f[...] = patch_ref[...].astype(F32)

        def widen(i, carry):
            copy(i).wait()
            chunk = pl.ds(pl.multiple_of(i * VOCAB_CHUNK, VOCAB_CHUNK), VOCAB_CHUNK)
            rows_f[chunk, :] = stage[chunk, :].astype(F32)
            return carry
        lax.fori_loop(0, chunks, widen, 0)

        replicas, stages, tokens = ids_ref.shape

        for z in range(stages):
            def put(r, carry):
                row = pl.multiple_of((z * replicas + r) * tokens, tokens)
                rows = patch_f[pl.ds(row, tokens), :]
                for t in range(tokens):
                    rows_f[pl.ds(ids_ref[r, stages - 1 - z, t], 1), :] = rows[t:t + 1, :]
                return carry
            lax.fori_loop(0, replicas, put, 0)

    @pl.when(step == 1)
    def _():
        for src, dst, buf, j in moves:
            pltpu.make_async_copy(src, buf, sem_g.at[j]).wait()
            buf[...] = buf[...] * scale
            pltpu.make_async_copy(buf, dst, sem_g.at[2 + j]).start()

    @pl.when(step == pl.num_programs(0) - 1)
    def _():
        for src, dst, buf, j in moves:
            pltpu.make_async_copy(buf, dst, sem_g.at[2 + j]).wait()

    pick = lax.broadcasted_iota(jnp.int32, (64, 128), 1) == lax.broadcasted_iota(jnp.int32, (64, 128), 0) + 64 * core
    sel = jnp.where(pick, scale, 0.0).astype(BF)
    for i in range(FINISH_BLOCK // VOCAB_CHUNK):
        start = pl.multiple_of(step * FINISH_BLOCK + i * VOCAB_CHUNK, VOCAB_CHUNK)
        block = rows_f[pl.ds(start, VOCAB_CHUNK), :].astype(BF)
        emb_out[:, i * VOCAB_CHUNK:(i + 1) * VOCAB_CHUNK] = lax.dot_general(sel, block, (((1,), (1,)), ((), ())), preferred_element_type=F32)


def solution(mesh):
    stages = mesh.shape['pp']
    replicas = mesh.shape['dp']

    def device_body(tok_ids, d_out, stored_x, w_in, w_out, acc_in, acc_out, acc_emb):
        layers, hid, ff = w_in.shape
        vocab = acc_emb.shape[1]
        tokens = d_out.shape[1]
        rows = tokens * stages
        ids = tok_ids[::-1].reshape(rows, 1)
        vm = pl.BlockSpec(memory_space=pltpu.VMEM)
        hbm = pl.BlockSpec(memory_space=pltpu.HBM)
        smem = pl.BlockSpec(memory_space=pltpu.SMEM)
        dma = pltpu.SemaphoreType.DMA
        slot_ids = pl.pallas_call(
            functools.partial(share_kernel, replicas),
            out_shape=jax.ShapeDtypeStruct((replicas, stages, tokens), jnp.int32),
            in_specs=[vm], out_specs=vm,
            scratch_shapes=[pltpu.VMEM((replicas, stages, tokens), jnp.int32), dma((replicas,)), dma((replicas,))],
            compiler_params=pltpu.CompilerParams(collective_id=1, has_side_effects=True),
            name='share_ids',
        )(tok_ids)
        touched = pl.pallas_call(
            gather_kernel,
            out_shape=jax.ShapeDtypeStruct((replicas * tokens, 4, 128), F32),
            in_specs=[smem, hbm], out_specs=vm, scratch_shapes=[pltpu.SemaphoreType.DMA],
            name='gather_rows',
        )(slot_ids, acc_emb.reshape(vocab, 4, 128))
        v = pltpu.VMEM
        dma = pltpu.SemaphoreType.DMA
        units = len(UNIT_ORDER)
        gin, gout, emb, patch = pl.pallas_call(
            functools.partial(comm_kernel, stages, layers, vocab),
            out_shape=(jax.ShapeDtypeStruct((layers, hid // 8, ff), F32), jax.ShapeDtypeStruct((layers, ff // 8, hid), F32),
                       jax.ShapeDtypeStruct((2 * stages, CHUNKS, VOCAB_CHUNK, 128), BF), jax.ShapeDtypeStruct((2 * stages, 128, 128), BF)),
            in_specs=[vm] * 5 + [hbm] * 5,
            out_specs=(vm, vm, hbm, hbm),
            scratch_shapes=[
                v((layers, rows, hid), BF), v((layers, rows, ff), BF), v((layers, rows, hid), BF), v((layers, rows, ff), BF), v((layers, rows, ff), F32),
                v((stages, tokens, hid), BF), v((stages, tokens, hid), BF), dma((2 * layers,)), dma((stages,)), dma((stages,)),
                v((layers, 2, 2, 2, 64, ff), BF), v((layers, 2, 2, 64, ff), BF), v((layers, 2, 64, ff), BF), v((layers, 64, ff), BF),
                v((layers, 2, 2, 2, 256, hid), BF), v((layers, 2, 2, 256, hid), BF), v((layers, 2, 256, hid), BF), v((layers, 256, hid), BF),
                v((CHUNKS, 2, 2, 2, VOCAB_CHUNK, 128), BF), v((CHUNKS, 2, 2, VOCAB_CHUNK, 128), BF), v((CHUNKS, 2, VOCAB_CHUNK, 128), BF), v((CHUNKS, VOCAB_CHUNK, 128), BF),
                v((2, 2, 2, 128, 128), BF), v((2, 2, 128, 128), BF), v((2, 128, 128), BF), v((128, 128), BF),
                v((2 * stages, CHUNKS, VOCAB_CHUNK, 128), BF), v((2 * stages, 128, 128), BF), v((stages, 4, tokens, 128), BF),
                v((2, 128, ff), F32), v((2, 512, hid), F32), v((2, VOCAB_CHUNK * 4, 128), F32),
                dma((2,)), dma((2,)), dma((2,)), dma((2 * stages, CHUNKS + 1)),
                dma((units,)), dma((units,)), dma((units,)), dma((units,)), dma((units,)), dma((units,)),
                dma((stages, stages)), dma((stages,)), dma((6, CHUNKS + 1)), dma((stages, CHUNKS)), dma((stages, CHUNKS + 1)), dma((stages, CHUNKS + 1)), dma((stages, CHUNKS + 1)),
            ],
            compiler_params=pltpu.CompilerParams(collective_id=0, has_side_effects=True, vmem_limit_bytes=67043328),
            name='reduce_exchange',
        )(ids, slot_ids, touched.reshape(-1, 128), d_out[0], stored_x[0], w_in.reshape(layers, 2, 2, 2, 64, ff), w_out.reshape(layers, 2, 2, 2, 256, hid), acc_in.reshape(layers, hid, ff), acc_out.reshape(layers, ff, hid), acc_emb.reshape(vocab * 4, 128))
        grad_emb, grad_in, grad_out = pl.pallas_call(
            functools.partial(finish_kernel, 1.0 / replicas),
            out_shape=(jax.ShapeDtypeStruct((64, vocab), F32), jax.ShapeDtypeStruct(gin.shape, F32), jax.ShapeDtypeStruct(gout.shape, F32)),
            grid=(2 * stages * HALF_VOCAB // FINISH_BLOCK,),
            in_specs=[smem, hbm, vm, hbm, hbm],
            out_specs=(pl.BlockSpec((64, FINISH_BLOCK), lambda i: (0, i)), hbm, hbm),
            scratch_shapes=[v((2 * stages * CHUNKS * VOCAB_CHUNK, 128), F32), v((stages * replicas * tokens, 128), F32),
                            v((2 * stages * CHUNKS * VOCAB_CHUNK, 128), BF), v(gin.shape, F32), v(gout.shape, F32), dma((2 * stages * CHUNKS,)), dma((4,))],
            compiler_params=pltpu.CompilerParams(vmem_limit_bytes=58 * 2 ** 20, dimension_semantics=('arbitrary',)),
            name='finish',
        )(slot_ids, emb.reshape(2 * stages * CHUNKS, VOCAB_CHUNK, 128), patch.reshape(-1, 128), gin, gout)
        return grad_in, grad_out, grad_emb.T

    return jax.shard_map(device_body, mesh=mesh, in_specs=(P(None, 'dp'), P('pp', 'dp', None), P('pp', None, 'dp', None), P('pp', None, None), P('pp', None, None), P('pp', 'dp', None, None), P('pp', 'dp', None, None), P('dp', None, None)), out_specs=(P('pp', 'dp', None), P('pp', 'dp', None), P(None, 'dp')), check_vma=False)
```
